768 devices in a mesh: dp: 24 (over y_hi, z), tensor: 32 (over y_lo, x, core).
Axes of the slice: x: 4, y: 8 (y_hi: 2, y_lo: 4; y = y_hi * 4 + y_lo), z: 12, core: 2. Of those that a mesh axis runs over, the one named last changes fastest.
Arguments:
- hidden_slots: bfloat16 [576, 16, 8192], P('dp', None, 'tensor'), may hold values from -6 to 6
- lengths: int32 [24, 24], replicated, may hold values from 1 to 16, 192 in all within a row
- owners: int32 [24, 24], replicated, may hold values from 0 to 23, as said below
- norm_gain: float32 [8192], replicated, may hold values from 0.25 to 1.75
- w_query: bfloat16 [8192, 8192], P(None, 'tensor'), may hold values from -0.0625 to 0.0625
- query_bias: float32 [8192], P('tensor'), may hold values from -3 to 3
- w_keyvalue: bfloat16 [8192, 2048], P('tensor'), may hold values from -0.0625 to 0.0625
- keyvalue_bias: float32 [2048], replicated, may hold values from -3 to 3
- grad_attention: bfloat16 [4608, 8192], P('dp', 'tensor'), may hold values from -6 to 6
Outputs:
- attention: bfloat16 [4608, 8192], P('dp', 'tensor')
- input_grad: bfloat16 [4608, 8192], P('dp', 'tensor')
The draws below stay inside these ranges and needn't reach their ends.
Inputs may be any that keep to these rules, and one draw needn't show every extreme that they name: `owners`: every owner appears exactly once in each row and exactly once in each column j, so each micro-batch takes one rollout from every owner and each owner holds exactly one rollout in each of its 24 slots. `lengths`: each row sums to 192, and its largest entry is 16.
All inputs are finite; a program needn't handle non-finite values.
Results may differ from the reference program's by a relative error of at most 0.013.
Values may be sent and summed in bfloat16 or wider, within the bound.
A program may use at most 64 MiB of HBM per device.

```python
import math
import jax
import jax.numpy as jnp
import numpy as np
from jax import lax

D = 8192
HEADS = 64
KV_HEADS = 8
HEAD_DIM = 128
TOK_DEV = 192
RPM = 24
LMAX = 16
SLOTS = 576
TOKENS = 4608
N_DP = 24


def draw_owners(key, part):
    first_key = jax.random.fold_in(key, 101)
    second_key = jax.random.fold_in(key, 202)
    third_key = jax.random.fold_in(key, 303)
    relabel = jax.random.permutation(first_key, N_DP)
    standing = jax.random.permutation(second_key, N_DP)
    shifts = jax.random.permutation(third_key, N_DP)[:RPM]
    owner_table = relabel[(standing[:, None] + shifts[None, :]) % N_DP]
    return owner_table.astype(jnp.int32)


def block_scale(key, dims, shards, least, top_value):
    def one(dim, parts):
        draws = jax.random.uniform(jax.random.fold_in(jax.random.fold_in(key, 6), dim), (parts,), jnp.float32, least / len(shards), top_value / len(shards))
        return jnp.repeat(jnp.exp(draws), dims[dim] // parts).reshape((-1,) + (1,) * (len(dims) - dim - 1))

    level = one(*shards[0])
    for cut in shards[1:]:
        level = level * one(*cut)
    return level


def length_profile(number_of, total, bound, skew):
    portions = [(1 << 20) // math.isqrt(rank ** skew) + 1 for rank in range(2, number_of + 1)]
    surplus, holding = total - bound - (number_of - 1), [1] * (number_of - 1)
    while surplus > 0:
        movable = [i for i in range(number_of - 1) if holding[i] < bound]
        whole, remaining = sum([portions[i] for i in movable]), surplus
        for i in movable:
            more = min(bound - holding[i], max(1, remaining * portions[i] // whole), surplus)
            holding[i] = holding[i] + more
            surplus = surplus - more
    return np.array([bound] + holding)


def uneven_parts(stream_key, number_of, total, bound, slope):
    if number_of == 2:
        one = jax.random.randint(stream_key, (), max(1, total - bound), min(bound, total - 1) + 1)
        return jnp.stack([one, total - one])
    sizes = jnp.asarray(length_profile(number_of, total, bound, slope), jnp.int32)
    twos = (number_of - 1) // 2
    source_of, taker = sizes[1:1 + 2 * twos:2], sizes[2:2 + 2 * twos:2]
    room = jnp.minimum(source_of - 1, bound - taker)
    moved = jax.random.randint(jax.random.fold_in(stream_key, 1), (twos,), 0, 1 << 20) % (room + 1)
    sizes = sizes.at[1:1 + 2 * twos:2].set(source_of - moved).at[2:2 + 2 * twos:2].set(taker + moved)
    return sizes[jax.random.permutation(jax.random.fold_in(stream_key, 2), number_of)]


def gaussian(stream_key, extent, spread, bound, split=(), kind=jnp.bfloat16):
    level = block_scale(stream_key, extent, split, -0.22, 0.18) if split else 1.0
    result = jax.random.normal(stream_key, extent, jnp.float32) * spread * level
    return jnp.minimum(jnp.maximum(result, -bound), bound).astype(kind)


def setup_inputs(seed: int = 0) -> dict:
    seeds = jax.random.split(jax.random.key(seed), 10)
    hidden_slots = gaussian(seeds[0], (SLOTS, LMAX, D), 1.0, 6.0, ((0, 24), (2, 32)))
    lengths = jax.vmap(lambda own: uneven_parts(own, RPM, TOK_DEV, LMAX, 2))(jax.random.split(seeds[1], N_DP)).reshape((N_DP, RPM)).astype(jnp.int32)
    owners = draw_owners(jax.random.fold_in(seeds[9], 71), 0)
    norm_gain = jnp.clip(1.0 + 0.15 * jax.random.normal(seeds[3], (D,), jnp.float32), 0.25, 1.75)
    w_query = gaussian(seeds[4], (D, HEADS * HEAD_DIM), D ** -0.5, 0.0625, ((1, 32),))
    query_bias = gaussian(seeds[5], (HEADS * HEAD_DIM,), 0.5, 3.0, ((0, 32),), jnp.float32)
    w_keyvalue = gaussian(seeds[6], (D, 2 * KV_HEADS * HEAD_DIM), D ** -0.5, 0.0625, ((0, 32),))
    keyvalue_bias = gaussian(seeds[7], (2 * KV_HEADS * HEAD_DIM,), 0.5, 3.0, (), jnp.float32)
    grad_attention = gaussian(seeds[8], (TOKENS, HEADS * HEAD_DIM), 1.0, 6.0, ((0, 24), (1, 32)))
    return {"hidden_slots": hidden_slots, "lengths": lengths, "owners": owners, "norm_gain": norm_gain, "w_query": w_query, "query_bias": query_bias, "w_keyvalue": w_keyvalue, "keyvalue_bias": keyvalue_bias, "grad_attention": grad_attention}


EPSILON = 1e-06
ROPE_BASE = 1000000.0

def packing(length_row, row_count):
    starts = jnp.cumsum(length_row) - length_row
    places = jnp.arange(row_count, dtype=jnp.int32)
    segment = lax.optimization_barrier(jnp.sum((places[:, None] >= starts[None, 1:]).astype(jnp.int32), axis=1))
    onehot = (segment[:, None] == jnp.arange(length_row.shape[0], dtype=jnp.int32)[None, :]).astype(jnp.int32)
    offset = places - lax.optimization_barrier(jnp.sum(onehot * starts[None, :], axis=1))
    return (segment, offset, onehot)

def tables(offset, head_width):
    halfway = head_width // 2
    frequency = ROPE_BASE ** (-2.0 * jnp.arange(halfway, dtype=jnp.float32) / head_width)
    angles = offset.astype(jnp.float32)[:, None] * frequency[None, :]
    angles = jnp.concatenate([angles, angles], axis=1)
    return (jnp.cos(angles)[:, None, :], jnp.sin(angles)[:, None, :])

def rotate(values, cosine, sine_table):
    halfway = values.shape[-1] // 2
    turned = jnp.concatenate([-values[..., halfway:], values[..., :halfway]], axis=-1)
    return values * cosine + turned * sine_table

def unrotate(gradient, cosine, sine_table):
    halfway = gradient.shape[-1] // 2
    scaled = gradient * sine_table
    turned = jnp.concatenate([scaled[..., halfway:], -scaled[..., :halfway]], axis=-1)
    return gradient * cosine + turned

def normalize(hidden, norm_gain):
    widened = hidden.astype(jnp.float32)
    inverse = lax.rsqrt(lax.optimization_barrier(jnp.mean(widened * widened, axis=1)) + EPSILON)
    normed = (widened * inverse[:, None] * norm_gain).astype(jnp.bfloat16)
    return (widened, inverse, normed)

def masked_softmax(scores, allowed):
    scores = jnp.where(allowed, scores, -1e+30)
    highest = lax.optimization_barrier(jnp.max(scores, axis=-1, keepdims=True))
    exponent = jnp.where(allowed, jnp.exp(scores - highest), 0.0)
    return exponent / lax.optimization_barrier(jnp.sum(exponent, axis=-1, keepdims=True))

def contract_last(operand, weights):
    return lax.dot_general(operand, weights, (((1,), (1,)), ((), ())), preferred_element_type=jnp.float32)

def reference(hidden_slots, lengths, owners, norm_gain, w_query, query_bias, w_keyvalue, keyvalue_bias, grad_attention):
    flat_rows = hidden_slots.reshape(N_DP * RPM * LMAX, D)
    group_size = HEADS // KV_HEADS
    kv_width = KV_HEADS * HEAD_DIM
    score_scale = HEAD_DIM ** (-0.5)

    def micro_batch(batch_index):
        length_row = lax.dynamic_index_in_dim(lengths, batch_index, 0, keepdims=False)
        owner_row = lax.dynamic_index_in_dim(owners, batch_index, 0, keepdims=False)
        segment, offset, onehot = packing(length_row, TOK_DEV)
        source = lax.optimization_barrier(jnp.sum(onehot * owner_row[None, :], axis=1))
        row_index = ((source * RPM + segment) * LMAX + offset).astype(jnp.int32)
        hidden = jnp.take(flat_rows, row_index, axis=0)
        upstream = lax.dynamic_slice_in_dim(grad_attention, (batch_index * TOK_DEV).astype(jnp.int32), TOK_DEV, 0)
        upstream_wide = upstream.reshape(TOK_DEV, HEADS, HEAD_DIM).astype(jnp.float32)
        widened, inverse, normed = normalize(hidden, norm_gain)
        query_full = jnp.dot(normed, w_query, preferred_element_type=jnp.float32) + query_bias
        keyvalue = jnp.dot(normed, w_keyvalue, preferred_element_type=jnp.float32) + keyvalue_bias
        cosine, sine_table = tables(offset, HEAD_DIM)
        query_rot = rotate(query_full.reshape(TOK_DEV, HEADS, HEAD_DIM), cosine, sine_table).astype(jnp.bfloat16)
        key_rot = rotate(keyvalue[:, :kv_width].reshape(TOK_DEV, KV_HEADS, HEAD_DIM), cosine, sine_table).astype(jnp.bfloat16)
        value_heads = keyvalue[:, kv_width:].reshape(TOK_DEV, KV_HEADS, HEAD_DIM).astype(jnp.bfloat16)
        key_wide = jnp.repeat(key_rot, group_size, axis=1).astype(jnp.float32)
        value_wide = jnp.repeat(value_heads, group_size, axis=1).astype(jnp.float32)
        query_wide = query_rot.astype(jnp.float32)
        places = jnp.arange(TOK_DEV, dtype=jnp.int32)
        allowed = (segment[:, None] == segment[None, :]) & (places[None, :] <= places[:, None])
        scores = jnp.einsum('qhd,khd->hqk', query_wide, key_wide) * score_scale
        attn_weights = masked_softmax(scores, allowed[None])
        low_weights = lax.optimization_barrier(attn_weights.astype(jnp.bfloat16)).astype(jnp.float32)
        attended = jnp.einsum('hqk,khd->qhd', low_weights, value_wide).astype(jnp.bfloat16)
        weight_grad = jnp.einsum('qhd,khd->hqk', upstream_wide, value_wide)
        value_part = jnp.einsum('hqk,qhd->khd', low_weights, upstream_wide)
        row_inner = lax.optimization_barrier(jnp.sum(attn_weights * weight_grad, axis=-1, keepdims=True))
        score_grad = lax.optimization_barrier((attn_weights * (weight_grad - row_inner) * score_scale).astype(jnp.bfloat16)).astype(jnp.float32)
        query_grad = unrotate(jnp.einsum('hqk,khd->qhd', score_grad, key_wide), cosine, sine_table).astype(jnp.bfloat16)
        key_part = jnp.einsum('hqk,qhd->khd', score_grad, query_wide)
        key_grad = unrotate(key_part.reshape(TOK_DEV, KV_HEADS, group_size, HEAD_DIM).sum(axis=2), cosine, sine_table).astype(jnp.bfloat16)
        value_grad = value_part.reshape(TOK_DEV, KV_HEADS, group_size, HEAD_DIM).sum(axis=2).astype(jnp.bfloat16)
        kv_grad = jnp.concatenate([key_grad.reshape(TOK_DEV, kv_width), value_grad.reshape(TOK_DEV, kv_width)], axis=1)
        normed_grad = contract_last(query_grad.reshape(TOK_DEV, HEADS * HEAD_DIM), w_query) + contract_last(kv_grad, w_keyvalue)
        scaled = norm_gain * normed_grad
        row_stat = lax.optimization_barrier(jnp.mean(scaled * widened, axis=1))
        input_grad = (inverse[:, None] * scaled - widened * (inverse ** 3 * row_stat)[:, None]).astype(jnp.bfloat16)
        return (attended.reshape(TOK_DEV, HEADS * HEAD_DIM), input_grad)
    results = lax.map(micro_batch, jnp.arange(N_DP, dtype=jnp.int32))
    return (results[0].reshape(TOKENS, HEADS * HEAD_DIM), results[1].reshape(TOKENS, D))
```

```python
import jax
import jax.numpy as jnp
import numpy as np
from jax import lax
from jax.experimental import pallas as pl
from jax.experimental.pallas import tpu as pltpu
from jax.sharding import PartitionSpec as P

D = 8192
HEADS = 64
KV_HEADS = 8
HEAD_DIM = 128
EPSILON = 1e-06
ROPE_BASE = 1000000.0
N_DP = 24
WINDOW = 16
ROWS = 192
HALF = 96
PART = 256
LANES = 32
HALF_DIM = HEAD_DIM // 2
SCALE = HEAD_DIM ** (-0.5)
MESH = pl.DeviceIdType.MESH
F32 = jnp.float32
BF16 = jnp.bfloat16
TREE_SLOTS = 35
GRAD_ROWS = HALF + 16
ORDER = (1, 2, 3, 0)


def mm(a, b):
    return jnp.dot(a, b, preferred_element_type=F32)


def mm_nt(a, b):
    return lax.dot_general(a, b, (((1,), (1,)), ((), ())), preferred_element_type=F32)


def mm_tn(a, b):
    return lax.dot_general(a, b, (((0,), (0,)), ((), ())), preferred_element_type=F32)


def exact_nt(a, b):
    return lax.dot_general(
        a, b, (((1,), (1,)), ((), ())), preferred_element_type=F32, precision=lax.Precision.HIGHEST
    )


def exact_mm(a, b):
    return lax.dot_general(
        a, b, (((1,), (0,)), ((), ())), preferred_element_type=F32, precision=lax.Precision.HIGHEST
    )


def iota(shape, dim):
    return lax.broadcasted_iota(jnp.int32, shape, dim)


class Links:
    def __init__(self, dp):
        self.dp = dp
        self.sent = []

    def copy(self, src, dst, send_sem, recv_sem, peer):
        return pltpu.make_async_remote_copy(
            src_ref=src,
            dst_ref=dst,
            send_sem=send_sem,
            recv_sem=recv_sem,
            device_id=(self.dp, peer),
            device_id_type=MESH,
        )

    def send(self, src, dst, send_sem, recv_sem, peer):
        one = self.copy(src, dst, send_sem, recv_sem, peer)
        one.start()
        self.sent.append(one)

    def wait(self, dst, send_sem, recv_sem, peer):
        self.copy(dst, dst, send_sem, recv_sem, peer).wait_recv()

    def drain(self):
        for one in self.sent:
            one.wait_send()


class Tree:
    def __init__(self, links, place, buffer, split, send_sems, recv_sems):
        self.links = links
        self.place = place
        self.buffer = buffer
        self.split = split
        self.ss = send_sems
        self.rs = recv_sems

    def block(self, tid):
        return self.buffer.at[tid]

    def part(self, tid, which):
        size = self.buffer.shape[1]
        if which == 0:
            return self.buffer.at[tid, pl.ds(0, self.split)]
        return self.buffer.at[tid, pl.ds(self.split, size - self.split)]

    def send(self, slot, ref, peer):
        self.links.send(ref, ref, self.ss.at[slot], self.rs.at[slot], peer)

    def wait(self, slot, ref, peer):
        self.links.wait(ref, self.ss.at[slot], self.rs.at[slot], peer)

    def spread(self, k):
        p = self.place
        ref = self.block(p.tid(p.ysrc(k), p.x, p.c))
        self.send(3 + k, ref, p.right)
        self.send(7 + k, ref, p.left)
        self.send(19 + k, ref, p.partner)

    def start(self):
        p = self.place
        ref = self.block(p.t)
        for k in (1, 2, 3):
            self.send(k - 1, ref, p.tid(p.ydst(k), p.x, p.c))
        self.spread(0)

    def step_y(self, k):
        p = self.place
        self.wait(k - 1, self.block(p.tid(p.ysrc(k), p.x, p.c)), p.tid(p.ysrc(k), p.x, p.c))
        self.spread(k)

    def step_x(self, k):
        p = self.place
        tid = p.tid(p.ysrc(k), p.xat(3), p.c)
        self.wait(3 + k, self.block(tid), p.left)
        self.send(11 + k, self.part(tid, 0), p.right)
        self.send(23 + k, self.block(tid), p.partner)
        tid = p.tid(p.ysrc(k), p.xat(1), p.c)
        self.wait(7 + k, self.block(tid), p.right)
        self.send(15 + k, self.part(tid, 1), p.left)
        self.send(27 + k, self.block(tid), p.partner)

    def step_far(self, k):
        p = self.place
        tid = p.tid(p.ysrc(k), p.xat(2), p.c)
        self.wait(11 + k, self.part(tid, 0), p.left)
        self.wait(15 + k, self.part(tid, 1), p.right)
        self.send(31 + k, self.block(tid), p.partner)

    def step_partner(self, k):
        p = self.place
        for j, shift in enumerate((0, 3, 1, 2)):
            tid = p.tid(p.ysrc(k), p.xat(shift), 1 - p.c)
            self.wait(19 + 4 * j + k, self.block(tid), p.partner)


class Place:
    def __init__(self):
        self.dp = lax.axis_index("dp")
        self.t = lax.axis_index("tensor")
        self.c = lax.rem(self.t, 2)
        self.x = lax.rem(lax.div(self.t, 2), 4)
        self.y = lax.div(self.t, 8)
        self.left = self.tid(self.y, self.xat(3), self.c)
        self.right = self.tid(self.y, self.xat(1), self.c)
        self.partner = self.tid(self.y, self.x, 1 - self.c)
        self.pair = lax.div(self.x, 2)
        self.kind = lax.rem(self.x, 2)
        self.mirror = self.tid(self.y, 3 - self.x, self.c)
        self.mate = self.tid(self.y, self.x + 1 - 2 * self.kind, self.c)

    def tid(self, y, x, c):
        return (y * 4 + x) * 2 + c

    def xat(self, shift):
        return lax.rem(self.x + shift, 4)

    def ydst(self, k):
        return lax.rem(self.y + k, 4)

    def ysrc(self, k):
        return lax.rem(self.y + 4 - k, 4)


def kernel(
    slots_in, lengths_in, owners_in, gain_in, wq_in, qbias_in, wkv_in, kvbias_in, up_in, cos_in, sin_in,
    att_out, grad_out,
    slots, lengths, owners, gain, wq, qbias, wkv, kvbias, up, cos16, sin16, att, grad,
    a_send, a_recv, full, acc, ssq,
    d0_send, d0_recv, d_own, d1_send, d1_recv, d2_send, d2_recv, d3_send, d3_recv, kvraw,
    cos_s, sin_s, q_grad, kv_f32, e1_send, e1_recv, e_sum, e2_send, e2_recv, ebuf, rs_rows, kvfull,
    f0_send, f0_recv, far_send, far_l, far_r, r_send, l_send, from_l, from_r, s_own, s_r, s_l, y_send, y_recv,
    local_sem, a_ss, a_rs, b_ss, b_rs, d_ss, d_rs, e_ss, e_rs, g_ss, g_rs, f_ss, f_rs,
):
    p = Place()
    dp, t, c = p.dp, p.t, p.c

    barrier = pltpu.get_barrier_semaphore()

    def greet(k, carry):
        pl.semaphore_signal(barrier, inc=1, device_id=(lax.rem(dp + k, N_DP), t), device_id_type=MESH)
        return carry

    lax.fori_loop(1, N_DP, greet, 0)
    for peer in (p.partner, p.left, p.right) + tuple(p.tid(p.ydst(k), p.x, c) for k in (1, 2, 3)):
        pl.semaphore_signal(barrier, inc=1, device_id=(dp, peer), device_id_type=MESH)

    pairs = (
        (owners_in, owners), (slots_in, slots), (lengths_in, lengths), (gain_in, gain), (wkv_in, wkv),
        (kvbias_in, kvbias), (qbias_in, qbias), (cos_in, cos16), (sin_in, sin16), (up_in, up), (wq_in, wq),
    )
    loads = [pltpu.make_async_copy(a, b, local_sem.at[i]) for i, (a, b) in enumerate(pairs)]
    for one in loads:
        one.start()

    total = N_DP * WINDOW
    row_of = (lax.div(iota((total, N_DP), 0), WINDOW) == iota((total, N_DP), 1)).astype(F32).astype(BF16)
    col_of = (lax.div(iota((N_DP, total), 1), WINDOW) == iota((N_DP, total), 0)).astype(F32).astype(BF16)
    same_row = lax.rem(iota((total, total), 0), WINDOW) == lax.rem(iota((total, total), 1), WINDOW)
    loads[0].wait()
    owner_f = owners[...].astype(F32)
    mine = (mm(row_of, owner_f.astype(BF16)) == dp.astype(F32)).astype(F32).astype(BF16)
    pick = jnp.where(same_row, mm(mine, col_of), 0.0).astype(BF16)
    loads[1].wait()
    outgoing = mm(pick, slots[...].reshape(total, PART)).astype(BF16).reshape(N_DP, WINDOW, PART)
    a_send[...] = outgoing
    a_recv[dp] = a_send[dp]
    pl.semaphore_wait(barrier, N_DP - 1 + 6)

    def rollout(src, dst, k, peer):
        return pltpu.make_async_remote_copy(
            src_ref=src, dst_ref=dst, send_sem=a_ss.at[k], recv_sem=a_rs.at[k], device_id=(peer, t), device_id_type=MESH
        )

    def send_rollout(k, carry):
        peer = lax.rem(dp + k, N_DP)
        rollout(a_send.at[peer], a_recv.at[dp], k, peer).start()
        return carry

    def wait_rollout(k, carry):
        peer = lax.rem(dp + N_DP - k, N_DP)
        rollout(a_recv.at[peer], a_recv.at[peer], k, peer).wait_recv()
        return carry

    def drain_rollout(k, carry):
        peer = lax.rem(dp + k, N_DP)
        rollout(a_send.at[peer], a_recv.at[dp], k, peer).wait_send()
        return carry

    lax.fori_loop(1, N_DP, send_rollout, 0)

    for one in loads[2:]:
        one.wait()
    length_row = jnp.broadcast_to(lengths[pl.ds(dp, 1), :].astype(F32), (ROWS, N_DP))
    owner_row = jnp.broadcast_to(owners[pl.ds(dp, 1), :].astype(F32), (ROWS, N_DP))
    before = (iota((N_DP, N_DP), 0) < iota((N_DP, N_DP), 1)).astype(F32).astype(BF16)
    starts = mm(length_row.astype(BF16), before)
    place = iota((ROWS, N_DP), 0).astype(F32)
    inside = (place >= starts) & (place < starts + length_row)
    start = jnp.sum(jnp.where(inside, starts, 0.0), axis=1, keepdims=True)
    source = jnp.sum(jnp.where(inside, owner_row, 0.0), axis=1, keepdims=True)
    offset = iota((ROWS, 1), 0).astype(F32) - start
    wanted = (source * WINDOW + offset).astype(jnp.int32)
    select = (iota((ROWS, total), 1) == wanted).astype(F32).astype(BF16)
    turn = (iota((ROWS, WINDOW), 1) == offset.astype(jnp.int32)).astype(F32)
    sign = jnp.where(iota((ROWS, HEAD_DIM), 1) < HALF_DIM, -1.0, 1.0)
    cos_s[...] = exact_mm(turn, cos16[...])
    sin_s[...] = exact_mm(turn, sin16[...])
    key_place = iota((ROWS, ROWS), 1)
    allowed = (key_place >= start.astype(jnp.int32)) & (key_place <= iota((ROWS, ROWS), 0))
    acc[...] = jnp.zeros_like(acc)
    ssq[...] = jnp.zeros_like(ssq)
    own_gain = jnp.concatenate([gain[pl.ds(2 * t, 1), :], gain[pl.ds(2 * t + 1, 1), :]], axis=1)

    lax.fori_loop(1, N_DP, wait_rollout, 0)
    hidden = mm(select, a_recv[...].reshape(total, PART))
    full[t] = hidden.astype(BF16)

    links = Links(dp)
    tree = Tree(links, p, full, HALF, b_ss, b_rs)
    tree.start()

    scaled_local = (hidden * own_gain).astype(BF16)

    def project(i, carry):
        for own, col in ((True, c * 1024 + i * 256), (False, (1 - c) * 1024 + i * 256)):
            value = mm(scaled_local, wkv[:, pl.ds(pl.multiple_of(col, 256), 256)])
            if own:
                d_own[2 * i] = value[:, :128]
                d_own[2 * i + 1] = value[:, 128:]
            else:
                d0_send[2 * i] = value[:, :128].astype(BF16)
                d0_send[2 * i + 1] = value[:, 128:].astype(BF16)
        return carry

    lax.fori_loop(0, 4, project, 0)
    links.send(d0_send, d0_recv, d_ss.at[0], d_rs.at[0], p.partner)

    def consume(core, k):
        def body(j, carry):
            tid = p.tid(p.ysrc(k), lax.rem(p.x + j, 4), core)
            block = full[tid].astype(F32)
            low, high = block[:, :128], block[:, 128:]
            ssq[...] += low * low + high * high
            scaled = jnp.concatenate(
                [low * gain[pl.ds(2 * tid, 1), :], high * gain[pl.ds(2 * tid + 1, 1), :]], axis=1
            ).astype(BF16)
            acc[...] += mm(scaled, wq[pl.ds(pl.multiple_of(tid * PART, PART), PART), :])
            return carry

        lax.fori_loop(0, 4, body, 0)

    tree.step_y(1)
    tree.step_x(0)
    links.wait(d0_recv, d_ss.at[0], d_rs.at[0], p.partner)
    for i in range(4):
        g = 2 * i + 1 - p.pair
        d1_send[i] = (d_own[g] + d0_recv[g].astype(F32)).astype(BF16)
    links.send(d1_send, d1_recv, d_ss.at[1], d_rs.at[1], p.mirror)
    tree.step_y(2)
    tree.step_x(1)
    tree.step_far(0)
    consume(c, 0)
    links.wait(d1_recv, d_ss.at[1], d_rs.at[1], p.mirror)

    def pair_sum(i):
        g = 2 * i + p.pair
        return d_own[g] + d0_recv[g].astype(F32) + d1_recv[i].astype(F32)

    for k in (1, 2, 3):
        d2_send[k] = pair_sum(p.ydst(k)).astype(BF16)
        links.send(d2_send.at[k], d2_recv.at[k], d_ss.at[1 + k], d_rs.at[1 + k], p.tid(p.ydst(k), p.x, c))
    tree.step_y(3)
    tree.step_x(2)
    tree.step_far(1)
    consume(c, 1)
    column = pair_sum(p.y)
    for k in (1, 2, 3):
        links.wait(d2_recv.at[k], d_ss.at[1 + k], d_rs.at[1 + k], p.tid(p.ysrc(k), p.x, c))
        column = column + d2_recv[k].astype(F32)
    d3_send[...] = column.astype(BF16)
    links.send(d3_send, d3_recv, d_ss.at[5], d_rs.at[5], p.mate)
    tree.step_x(3)
    tree.step_far(2)
    tree.step_partner(0)
    consume(1 - c, 0)
    consume(c, 2)
    links.wait(d3_recv, d_ss.at[5], d_rs.at[5], p.mate)
    kvraw[c] = column + d3_recv[...].astype(F32)
    links.send(kvraw.at[c], kvraw.at[c], d_ss.at[6], d_rs.at[6], p.partner)
    tree.step_partner(1)
    consume(1 - c, 1)
    tree.step_far(3)
    consume(c, 3)
    tree.step_partner(2)
    consume(1 - c, 2)
    tree.step_partner(3)
    consume(1 - c, 3)
    links.wait(kvraw.at[1 - c], d_ss.at[6], d_rs.at[6], p.partner)

    cosine, sine = cos_s[...], sin_s[...]
    inverse = lax.rsqrt(jnp.sum(ssq[...], axis=1, keepdims=True) * (1.0 / D) + EPSILON)

    def rotate(u):
        return u * cosine + pltpu.roll(u, HALF_DIM, 1) * (sign * sine)

    def unrotate(z, cosine, sine, sign):
        return z * cosine - pltpu.roll(z * sine, HALF_DIM, 1) * sign

    group = p.y * 2 + p.pair
    key_raw, value_raw = kvraw[0], kvraw[1]
    key = rotate(inverse * key_raw + kvbias[pl.ds(group, 1), :]).astype(BF16)
    value = (inverse * value_raw + kvbias[pl.ds(KV_HEADS + group, 1), :]).astype(BF16)
    query = jnp.concatenate(
        [rotate(inverse * acc[:, h * 128 : h * 128 + 128] + qbias[h : h + 1, :]).astype(BF16) for h in (0, 1)], axis=0
    )
    upstream = jnp.concatenate([up[:, :128], up[:, 128:]], axis=0)
    both = jnp.concatenate([allowed.astype(F32), allowed.astype(F32)], axis=0) > 0.5
    scores = jnp.where(both, mm_nt(query, key) * SCALE, -1e30)
    highest = jnp.max(scores, axis=1, keepdims=True)
    exponent = jnp.where(both, jnp.exp(scores - highest), 0.0)
    weights = exponent / jnp.sum(exponent, axis=1, keepdims=True)
    low = weights.astype(BF16)
    attended = mm(low, value).astype(BF16)
    att[:, :128] = attended[:ROWS]
    att[:, 128:] = attended[ROWS:]
    att_copy = pltpu.make_async_copy(att, att_out, local_sem.at[11])
    att_copy.start()
    weight_grad = mm_nt(upstream, value)
    inner = jnp.sum(weights * weight_grad, axis=1, keepdims=True)
    score_grad = (weights * (weight_grad - inner) * SCALE).astype(BF16)
    kv_f32[0] = mm_tn(score_grad, query)
    kv_f32[1] = mm_tn(low, upstream)
    e1_send[...] = kv_f32[...].astype(BF16)
    other = pl.multiple_of((1 - c) * HALF, HALF)
    links.send(e1_send.at[:, pl.ds(other, HALF), :], e1_recv, g_ss.at[0], g_rs.at[0], p.partner)
    query_grad = mm(score_grad, key)
    for h in (0, 1):
        piece = unrotate(query_grad[h * ROWS : h * ROWS + ROWS], cosine, sine, sign).astype(BF16)
        q_grad[:, h * 128 : h * 128 + 128] = piece
        product = piece.astype(F32) * acc[:, h * 128 : h * 128 + 128]
        if h == 0:
            rs_rows[pl.ds(0, ROWS), :] = product
        else:
            rs_rows[pl.ds(0, ROWS), :] += product
    rs_rows[pl.ds(ROWS, 64), :] = jnp.zeros((64, 128), F32)

    def partial(k, shift, core):
        tid = p.tid(p.ydst(k), lax.rem(p.x + shift, 4), core)
        return mm_nt(q_grad[...], wq[pl.ds(pl.multiple_of(tid * PART, PART), PART), :])

    def f_cores(k):
        def body(j, carry):
            f0_send[k, j] = partial(k, j, 1 - c).astype(BF16)
            return carry

        lax.fori_loop(0, 4, body, 0)
        links.send(f0_send.at[k], f0_recv.at[k], f_ss.at[k], f_rs.at[k], p.partner)

    top, bottom = pl.ds(0, HALF), pl.ds(HALF, HALF)

    def f_first(k):
        links.wait(f0_recv.at[k], f_ss.at[k], f_rs.at[k], p.partner)
        far_send[k] = (partial(k, 2, c) + f0_recv[k, 2].astype(F32)).astype(BF16)
        links.send(far_send.at[k, top], far_l.at[k], f_ss.at[4 + k], f_rs.at[4 + k], p.right)
        links.send(far_send.at[k, bottom], far_r.at[k], f_ss.at[8 + k], f_rs.at[8 + k], p.left)
        value = partial(k, 1, c) + f0_recv[k, 1].astype(F32)
        r_send[k, bottom] = value[HALF:].astype(BF16)
        links.send(r_send.at[k, bottom], from_l.at[k, bottom], f_ss.at[12 + k], f_rs.at[12 + k], p.right)
        s_r[k] = value[:HALF]
        value = partial(k, 3, c) + f0_recv[k, 3].astype(F32)
        l_send[k, top] = value[:HALF].astype(BF16)
        links.send(l_send.at[k, top], from_r.at[k, top], f_ss.at[16 + k], f_rs.at[16 + k], p.left)
        s_l[k] = value[HALF:]
        s_own[k] = partial(k, 0, c) + f0_recv[k, 0].astype(F32)

    def f_second(k):
        links.wait(far_l.at[k], f_ss.at[4 + k], f_rs.at[4 + k], p.left)
        r_send[k, top] = (s_r[k] + far_l[k].astype(F32)).astype(BF16)
        links.send(r_send.at[k, top], from_l.at[k, top], f_ss.at[20 + k], f_rs.at[20 + k], p.right)
        links.wait(far_r.at[k], f_ss.at[8 + k], f_rs.at[8 + k], p.right)
        l_send[k, bottom] = (s_l[k] + far_r[k].astype(F32)).astype(BF16)
        links.send(l_send.at[k, bottom], from_r.at[k, bottom], f_ss.at[24 + k], f_rs.at[24 + k], p.left)

    def f_third(k):
        links.wait(from_l.at[k, bottom], f_ss.at[12 + k], f_rs.at[12 + k], p.left)
        links.wait(from_r.at[k, top], f_ss.at[16 + k], f_rs.at[16 + k], p.right)
        links.wait(from_l.at[k, top], f_ss.at[20 + k], f_rs.at[20 + k], p.left)
        links.wait(from_r.at[k, bottom], f_ss.at[24 + k], f_rs.at[24 + k], p.right)
        value = s_own[k] + from_l[k].astype(F32) + from_r[k].astype(F32)
        if k == 0:
            s_own[k] = value
        else:
            y_send[k] = value.astype(BF16)
            links.send(
                y_send.at[k], y_recv.at[k], f_ss.at[28 + k], f_rs.at[28 + k], p.tid(p.ydst(k), p.x, c)
            )

    grads = Tree(links, p, ebuf, 64, e_ss, e_rs)
    f_cores(1)
    f_cores(2)
    links.wait(e1_recv, g_ss.at[0], g_rs.at[0], p.partner)
    mine_rows = pl.ds(pl.multiple_of(c * HALF, HALF), HALF)
    e_sum[...] = kv_f32[:, mine_rows, :] + e1_recv[...].astype(F32)
    e2_send[...] = e_sum[...].astype(BF16)
    links.send(e2_send.at[1 - p.kind], e2_recv, g_ss.at[1], g_rs.at[1], p.mate)
    f_first(1)
    f_cores(3)
    f_first(2)
    links.wait(e2_recv, g_ss.at[1], g_rs.at[1], p.mate)
    value_side = p.kind.astype(F32)
    half_sign = sign[:HALF]
    finished = unrotate(
        e_sum[p.kind] + e2_recv[...].astype(F32),
        cos_s[mine_rows, :] * (1.0 - value_side) + value_side,
        sin_s[mine_rows, :] * (1.0 - value_side),
        half_sign,
    ).astype(BF16)
    rs_rows[mine_rows, :] += finished.astype(F32) * kvraw[p.kind, mine_rows, :]
    ones = jnp.ones((8, 128), F32)
    stat = jnp.concatenate([exact_nt(ones, rs_rows[0:128, :]), exact_nt(ones, rs_rows[128:256, :])], axis=0)
    coarse = stat.astype(BF16).astype(F32)
    ebuf[t, pl.ds(0, HALF)] = finished
    ebuf[t, pl.ds(HALF, 16)] = jnp.where(lax.rem(iota((16, 128), 0), 2) == 0, coarse, stat - coarse).astype(BF16)
    grads.start()
    f_cores(0)
    f_second(1)
    f_first(3)
    f_second(2)
    f_third(1)
    grads.step_y(1)
    f_first(0)
    f_second(3)
    f_third(2)
    grads.step_y(2)
    grads.step_x(0)
    f_second(0)
    grads.step_y(3)
    grads.step_x(1)
    grads.step_far(0)
    f_third(3)
    grads.step_x(2)
    grads.step_far(1)
    grads.step_x(3)
    grads.step_far(2)
    grads.step_far(3)
    f_third(0)
    for k in range(4):
        grads.step_partner(k)

    def place_grad(tid, carry):
        core = lax.rem(tid, 2)
        xs = lax.rem(lax.div(tid, 2), 4)
        ys = lax.div(tid, 8)
        col = lax.rem(xs, 2) * 1024 + (ys * 2 + lax.div(xs, 2)) * 128
        kvfull[pl.ds(pl.multiple_of(core * HALF, HALF), HALF), pl.ds(pl.multiple_of(col, 128), 128)] = ebuf[
            tid, pl.ds(0, HALF)
        ]
        return carry + ebuf[tid, pl.ds(HALF, 16)].astype(F32)

    stats = lax.fori_loop(0, LANES, place_grad, jnp.zeros((16, 128), F32))
    key_value_part = mm_nt(kvfull[...], wkv[...])
    eye = iota((128, 128), 0) == iota((128, 128), 1)

    def upright(row):
        return jnp.sum(jnp.where(eye, jnp.broadcast_to(row, (128, 128)), 0.0), axis=1, keepdims=True)

    row_stat = jnp.concatenate(
        [upright(stats[0:1] + stats[1:2]), upright(stats[8:9] + stats[9:10])[: ROWS - 128]], axis=0
    ) * (1.0 / D)
    normed_grad = s_own[0] + key_value_part
    for k in (1, 2, 3):
        links.wait(y_recv.at[k], f_ss.at[28 + k], f_rs.at[28 + k], p.tid(p.ysrc(k), p.x, c))
        normed_grad = normed_grad + y_recv[k].astype(F32)
    own_gain = jnp.concatenate([gain[pl.ds(2 * t, 1), :], gain[pl.ds(2 * t + 1, 1), :]], axis=1)
    grad[...] = (
        inverse * (own_gain * normed_grad)
        - full[t].astype(F32) * (inverse * inverse * inverse * row_stat)
    ).astype(BF16)
    grad_copy = pltpu.make_async_copy(grad, grad_out, local_sem.at[12])
    grad_copy.start()
    lax.fori_loop(1, N_DP, drain_rollout, 0)
    links.drain()
    att_copy.wait()
    grad_copy.wait()


def on_device(
    hidden_slots, lengths, owners, norm_gain, w_query, query_bias, w_keyvalue, keyvalue_bias, grad_attention
):
    frequency = ROPE_BASE ** (-2.0 * np.arange(HALF_DIM, dtype=np.float32) / HEAD_DIM)
    angles = np.arange(WINDOW, dtype=np.float32)[:, None] * frequency[None, :].astype(np.float32)
    angles = np.concatenate([angles, angles], axis=1)
    cosine = jnp.asarray(np.cos(angles), F32)
    sine = jnp.asarray(np.sin(angles), F32)
    operands = (
        hidden_slots, lengths, owners, norm_gain.reshape(64, 128), w_query, query_bias.reshape(2, 128),
        w_keyvalue, keyvalue_bias.reshape(16, 128), grad_attention, cosine, sine,
    )

    def v(*shape, dtype=BF16):
        return pltpu.VMEM(shape, dtype)

    def dma(n):
        return pltpu.SemaphoreType.DMA((n,))

    scratch = [pltpu.VMEM(one.shape, one.dtype) for one in operands]
    scratch += [v(ROWS, PART), v(ROWS, PART)]
    scratch += [
        v(N_DP, WINDOW, PART), v(N_DP, WINDOW, PART), v(LANES, ROWS, PART), v(ROWS, PART, dtype=F32),
        v(ROWS, 128, dtype=F32),
    ]
    scratch += [
        v(8, ROWS, 128), v(8, ROWS, 128), v(8, ROWS, 128, dtype=F32), v(4, ROWS, 128), v(4, ROWS, 128),
        v(4, ROWS, 128), v(4, ROWS, 128), v(ROWS, 128), v(ROWS, 128), v(2, ROWS, 128, dtype=F32),
    ]
    scratch += [
        v(ROWS, 128, dtype=F32), v(ROWS, 128, dtype=F32), v(ROWS, PART), v(2, ROWS, 128, dtype=F32),
        v(2, ROWS, 128), v(2, HALF, 128), v(2, HALF, 128, dtype=F32), v(2, HALF, 128), v(HALF, 128),
        v(LANES, GRAD_ROWS, 128), v(256, 128, dtype=F32), v(ROWS, 2048),
    ]
    scratch += [
        v(4, 4, ROWS, PART), v(4, 4, ROWS, PART), v(4, ROWS, PART), v(4, HALF, PART), v(4, HALF, PART),
        v(4, ROWS, PART), v(4, ROWS, PART), v(4, ROWS, PART), v(4, ROWS, PART), v(4, ROWS, PART, dtype=F32),
        v(4, HALF, PART, dtype=F32), v(4, HALF, PART, dtype=F32), v(4, ROWS, PART), v(4, ROWS, PART),
    ]
    scratch += [
        dma(13), dma(N_DP), dma(N_DP), dma(TREE_SLOTS), dma(TREE_SLOTS), dma(7), dma(7),
        dma(TREE_SLOTS), dma(TREE_SLOTS), dma(2), dma(2), dma(32), dma(32),
    ]
    shape = jax.ShapeDtypeStruct((ROWS, PART), BF16)
    return pl.pallas_call(
        kernel,
        out_shape=(shape, shape),
        in_specs=[pl.BlockSpec(memory_space=pl.ANY)] * len(operands),
        out_specs=[pl.BlockSpec(memory_space=pl.ANY)] * 2,
        scratch_shapes=scratch,
        compiler_params=pltpu.CompilerParams(
            collective_id=0, has_side_effects=True, vmem_limit_bytes=60 * 1024 * 1024
        ),
        name="step",
    )(*operands)


def solution(mesh):
    in_specs = (
        P("dp", None, "tensor"),
        P(),
        P(),
        P(),
        P(None, "tensor"),
        P("tensor"),
        P("tensor", None),
        P(),
        P("dp", "tensor"),
    )
    out_specs = (P("dp", "tensor"), P("dp", "tensor"))
    return jax.shard_map(on_device, mesh=mesh, in_specs=in_specs, out_specs=out_specs, check_vma=False)
```

```python
import jax
import jax.numpy as jnp
import numpy as np
from jax import lax
from jax.experimental import pallas as pl
from jax.experimental.pallas import tpu as pltpu
from jax.sharding import PartitionSpec as P

D = 8192
HEADS = 64
KV_HEADS = 8
HEAD_DIM = 128
EPSILON = 1e-06
ROPE_BASE = 1000000.0
N_DP = 24
WINDOW = 16
ROWS = 192
HALF = 96
PART = 256
LANES = 32
HALF_DIM = HEAD_DIM // 2
SCALE = HEAD_DIM ** (-0.5)
MESH = pl.DeviceIdType.MESH
F32 = jnp.float32
BF16 = jnp.bfloat16
TREE_SLOTS = 39
GRAD_ROWS = ROWS + 16
ORDER = (1, 2, 3, 0)


def mm(a, b):
    return jnp.dot(a, b, preferred_element_type=F32)


def mm_nt(a, b):
    return lax.dot_general(a, b, (((1,), (1,)), ((), ())), preferred_element_type=F32)


def mm_tn(a, b):
    return lax.dot_general(a, b, (((0,), (0,)), ((), ())), preferred_element_type=F32)


def exact_nt(a, b):
    return lax.dot_general(
        a, b, (((1,), (1,)), ((), ())), preferred_element_type=F32, precision=lax.Precision.HIGHEST
    )


def exact_mm(a, b):
    return lax.dot_general(
        a, b, (((1,), (0,)), ((), ())), preferred_element_type=F32, precision=lax.Precision.HIGHEST
    )


def iota(shape, dim):
    return lax.broadcasted_iota(jnp.int32, shape, dim)


class Links:
    def __init__(self, dp):
        self.dp = dp
        self.sent = []

    def copy(self, src, dst, send_sem, recv_sem, peer):
        return pltpu.make_async_remote_copy(
            src_ref=src,
            dst_ref=dst,
            send_sem=send_sem,
            recv_sem=recv_sem,
            device_id=(self.dp, peer),
            device_id_type=MESH,
        )

    def send(self, src, dst, send_sem, recv_sem, peer):
        one = self.copy(src, dst, send_sem, recv_sem, peer)
        one.start()
        self.sent.append(one)

    def wait(self, dst, send_sem, recv_sem, peer):
        self.copy(dst, dst, send_sem, recv_sem, peer).wait_recv()

    def drain(self):
        for one in self.sent:
            one.wait_send()


class Tree:
    def __init__(self, links, place, buffer, cuts, send_sems, recv_sems):
        self.links = links
        self.place = place
        self.buffer = buffer
        self.cuts = cuts
        self.ss = send_sems
        self.rs = recv_sems

    def block(self, tid):
        return self.buffer.at[tid]

    def part(self, tid, which):
        low, high = self.cuts
        begin, size = ((0, low), (low, high - low), (high, self.buffer.shape[1] - high))[which]
        return self.buffer.at[tid, pl.ds(begin, size)]

    def send(self, slot, ref, peer):
        self.links.send(ref, ref, self.ss.at[slot], self.rs.at[slot], peer)

    def wait(self, slot, ref, peer):
        self.links.wait(ref, self.ss.at[slot], self.rs.at[slot], peer)

    def spread(self, k):
        p = self.place
        ref = self.block(p.tid(p.ysrc(k), p.x, p.c))
        self.send(3 + k, ref, p.right)
        self.send(7 + k, ref, p.left)
        self.send(19 + k, ref, p.partner)

    def start(self):
        p = self.place
        ref = self.block(p.t)
        for k in (1, 2, 3):
            self.send(k - 1, ref, p.tid(p.ydst(k), p.x, p.c))
        self.spread(0)

    def step_y(self, k):
        p = self.place
        self.wait(k - 1, self.block(p.tid(p.ysrc(k), p.x, p.c)), p.tid(p.ysrc(k), p.x, p.c))
        self.spread(k)

    def step_x(self, k):
        p = self.place
        left = p.tid(p.ysrc(k), p.xat(3), p.c)
        right = p.tid(p.ysrc(k), p.xat(1), p.c)
        self.wait(3 + k, self.block(left), p.left)
        self.send(11 + k, self.part(left, 0), p.right)
        self.wait(7 + k, self.block(right), p.right)
        self.send(15 + k, self.part(right, 2), p.left)
        self.send(35 + k, self.part(p.tid(p.ysrc(k), 3 - p.x, p.c), 1), p.mate)
        self.send(23 + k, self.block(left), p.partner)
        self.send(27 + k, self.block(right), p.partner)

    def step_far(self, k):
        p = self.place
        tid = p.tid(p.ysrc(k), p.xat(2), p.c)
        self.wait(11 + k, self.part(tid, 0), p.left)
        self.wait(15 + k, self.part(tid, 2), p.right)
        self.wait(35 + k, self.part(tid, 1), p.mate)
        self.send(31 + k, self.block(tid), p.partner)

    def partner_wait(self, k, which):
        p = self.place
        for j, shift in enumerate((0, 3, 1, 2)):
            if j in which:
                tid = p.tid(p.ysrc(k), p.xat(shift), 1 - p.c)
                self.wait(19 + 4 * j + k, self.block(tid), p.partner)

    def partner_near(self, k):
        self.partner_wait(k, (0, 1, 2))

    def partner_far(self, k):
        self.partner_wait(k, (3,))


class Place:
    def __init__(self):
        self.dp = lax.axis_index("dp")
        self.t = lax.axis_index("tensor")
        self.c = lax.rem(self.t, 2)
        self.x = lax.rem(lax.div(self.t, 2), 4)
        self.y = lax.div(self.t, 8)
        self.left = self.tid(self.y, self.xat(3), self.c)
        self.right = self.tid(self.y, self.xat(1), self.c)
        self.partner = self.tid(self.y, self.x, 1 - self.c)
        self.pair = lax.div(self.x, 2)
        self.kind = lax.rem(self.x, 2)
        self.mirror = self.tid(self.y, 3 - self.x, self.c)
        self.mirror_other = self.tid(self.y, 3 - self.x, 1 - self.c)
        self.row_index = self.x * 2 + self.c
        self.mate = self.tid(self.y, self.x + 1 - 2 * self.kind, self.c)

    def in_row(self, j):
        return self.y * 8 + lax.rem(self.row_index + j, 8)

    def tid(self, y, x, c):
        return (y * 4 + x) * 2 + c

    def xat(self, shift):
        return lax.rem(self.x + shift, 4)

    def ydst(self, k):
        if k == 3:
            return 3 - self.y
        if k == 2:
            return self.y + 2 - 4 * lax.div(self.y, 2)
        if k == 1:
            return self.y + 1 - 2 * lax.rem(self.y, 2)
        return self.y

    def ysrc(self, k):
        return self.ydst(k)


def kernel(
    slots_in, lengths_in, owners_in, gain_in, wq_in, qbias_in, wkv_in, kvbias_in, up_in, cos_in, sin_in,
    att_out, grad_out,
    slots, lengths, owners, gain, wq, qbias, kvbias, up, cos16, sin16, att, grad,
    a_send, a_recv, full, acc, ssq,
    w_own, w_far, d_own, d2_send, d2_recv, d3_send, d3_recv, kvraw,
    cos_s, sin_s, q_grad, kv_f32, e1_send, e1_recv, e2_send, e2_recv, ebuf, rs_rows, rs_all, kv_part, products_s,
    f0_send, f0_recv, far_send, far_l, far_r, r_send, l_send, from_l, from_r, s_own, s_r, s_l, y_send, y_recv,
    local_sem, a_ss, a_rs, b_ss, b_rs, d_ss, d_rs, e_ss, e_rs, r_ss, r_rs, c_ss, c_rs, f_ss, f_rs,
):
    p = Place()
    dp, t, c = p.dp, p.t, p.c

    barrier = pltpu.get_barrier_semaphore()

    def greet(k, carry):
        pl.semaphore_signal(barrier, inc=1, device_id=(lax.rem(dp + k, N_DP), t), device_id_type=MESH)
        return carry

    lax.fori_loop(1, N_DP, greet, 0)
    for peer in tuple(p.in_row(j) for j in range(1, 8)) + tuple(p.tid(p.ydst(k), p.x, c) for k in (1, 2, 3)):
        pl.semaphore_signal(barrier, inc=1, device_id=(dp, peer), device_id_type=MESH)

    pairs = (
        (owners_in, owners), (slots_in, slots), (lengths_in, lengths), (gain_in, gain),
        (kvbias_in, kvbias), (qbias_in, qbias), (cos_in, cos16), (sin_in, sin16), (up_in, up), (wq_in, wq),
    )
    loads = [pltpu.make_async_copy(a, b, local_sem.at[i]) for i, (a, b) in enumerate(pairs)]
    for kind in (0, 1):
        for pair in (0, 1):
            for i in range(4):
                loads.append(
                    pltpu.make_async_copy(
                        wkv_in.at[:, pl.ds(kind * 1024 + (2 * i + pair) * 128, 128)],
                        w_own.at[kind, pair, :, pl.ds(i * 128, 128)],
                        local_sem.at[12 + kind * 8 + pair * 4 + i],
                    )
                )
    for one in loads:
        one.start()

    total = N_DP * WINDOW
    row_of = (lax.div(iota((total, N_DP), 0), WINDOW) == iota((total, N_DP), 1)).astype(F32).astype(BF16)
    col_of = (lax.div(iota((N_DP, total), 1), WINDOW) == iota((N_DP, total), 0)).astype(F32).astype(BF16)
    same_row = lax.rem(iota((total, total), 0), WINDOW) == lax.rem(iota((total, total), 1), WINDOW)
    loads[0].wait()
    owner_f = owners[...].astype(F32)
    mine = (mm(row_of, owner_f.astype(BF16)) == dp.astype(F32)).astype(F32).astype(BF16)
    pick = jnp.where(same_row, mm(mine, col_of), 0.0).astype(BF16)
    loads[1].wait()
    outgoing = mm(pick, slots[...].reshape(total, PART)).astype(BF16).reshape(N_DP, WINDOW, PART)
    a_send[...] = outgoing
    a_recv[dp] = a_send[dp]
    pl.semaphore_wait(barrier, N_DP - 1 + 10)

    def rollout(src, dst, k, peer):
        return pltpu.make_async_remote_copy(
            src_ref=src, dst_ref=dst, send_sem=a_ss.at[k], recv_sem=a_rs.at[k], device_id=(peer, t), device_id_type=MESH
        )

    def send_rollout(k, carry):
        peer = lax.rem(dp + k, N_DP)
        rollout(a_send.at[peer], a_recv.at[dp], k, peer).start()
        return carry

    def wait_rollout(k, carry):
        peer = lax.rem(dp + N_DP - k, N_DP)
        rollout(a_recv.at[peer], a_recv.at[peer], k, peer).wait_recv()
        return carry

    def drain_rollout(k, carry):
        peer = lax.rem(dp + k, N_DP)
        rollout(a_send.at[peer], a_recv.at[dp], k, peer).wait_send()
        return carry

    lax.fori_loop(1, N_DP, send_rollout, 0)

    for one in loads[2:]:
        one.wait()
    links = Links(dp)
    links.send(w_own.at[1 - c, p.pair], w_far.at[0], d_ss.at[0], d_rs.at[0], p.partner)
    links.send(w_own.at[c, 1 - p.pair], w_far.at[1], d_ss.at[1], d_rs.at[1], p.mirror)
    links.send(w_own.at[1 - c, 1 - p.pair], w_far.at[2], d_ss.at[7], d_rs.at[7], p.mirror_other)

    length_row = jnp.broadcast_to(lengths[pl.ds(dp, 1), :].astype(F32), (ROWS, N_DP))
    owner_row = jnp.broadcast_to(owners[pl.ds(dp, 1), :].astype(F32), (ROWS, N_DP))
    before = (iota((N_DP, N_DP), 0) < iota((N_DP, N_DP), 1)).astype(F32).astype(BF16)
    starts = mm(length_row.astype(BF16), before)
    place = iota((ROWS, N_DP), 0).astype(F32)
    inside = (place >= starts) & (place < starts + length_row)
    start = jnp.sum(jnp.where(inside, starts, 0.0), axis=1, keepdims=True)
    source = jnp.sum(jnp.where(inside, owner_row, 0.0), axis=1, keepdims=True)
    offset = iota((ROWS, 1), 0).astype(F32) - start
    wanted = (source * WINDOW + offset).astype(jnp.int32)
    select = (iota((ROWS, total), 1) == wanted).astype(F32).astype(BF16)
    turn = (iota((ROWS, WINDOW), 1) == offset.astype(jnp.int32)).astype(F32)
    sign = jnp.where(iota((ROWS, HEAD_DIM), 1) < HALF_DIM, -1.0, 1.0)
    cos_s[...] = exact_mm(turn, cos16[...])
    sin_s[...] = exact_mm(turn, sin16[...])
    key_place = iota((ROWS, ROWS), 1)
    allowed = (key_place >= start.astype(jnp.int32)) & (key_place <= iota((ROWS, ROWS), 0))
    acc[...] = jnp.zeros_like(acc)
    ssq[...] = jnp.zeros_like(ssq)
    kv_part[...] = jnp.zeros_like(kv_part)

    lax.fori_loop(1, N_DP, wait_rollout, 0)
    hidden = mm(select, a_recv[...].reshape(total, PART))
    full[t] = hidden.astype(BF16)

    tree = Tree(links, p, full, (80, 112), b_ss, b_rs)
    tree.start()

    def scaled(tid):
        block = full[tid].astype(F32)
        low, high = block[:, :128], block[:, 128:]
        value = jnp.concatenate([low * gain[pl.ds(2 * tid, 1), :], high * gain[pl.ds(2 * tid + 1, 1), :]], axis=1)
        return value.astype(BF16), low * low + high * high

    def consume(*items):
        total, squares = None, None
        for core, k, shifts in items:
            for shift in shifts:
                tid = p.tid(p.ysrc(k), p.xat(shift), core)
                value, square = scaled(tid)
                part = mm(value, wq[pl.ds(pl.multiple_of(tid * PART, PART), PART), :])
                total = part if total is None else total + part
                squares = square if squares is None else squares + square
        ssq[...] += squares
        acc[...] += total

    near, far = (0, 1, 3), (2,)
    tree.step_x(0)
    tree.step_y(1)
    tree.partner_near(0)
    links.wait(w_far.at[0], d_ss.at[0], d_rs.at[0], p.partner)
    links.wait(w_far.at[1], d_ss.at[1], d_rs.at[1], p.mirror)
    links.wait(w_far.at[2], d_ss.at[7], d_rs.at[7], p.mirror_other)
    weights_of = ((t, w_own.at[c, p.pair]), (p.partner, w_far.at[0]), (p.mirror, w_far.at[1]), (p.mirror_other, w_far.at[2]))
    low_sum, high_sum = jnp.zeros((ROWS, 256), F32), jnp.zeros((ROWS, 256), F32)
    for tid, ref in weights_of:
        value = scaled(tid)[0]
        low_sum = low_sum + mm(value, ref[:, :256])
        high_sum = high_sum + mm(value, ref[:, 256:])
    for i, value in enumerate((low_sum, high_sum)):
        d_own[2 * i] = value[:, :128]
        d_own[2 * i + 1] = value[:, 128:]
    for k in (1, 2, 3):
        d2_send[k] = d_own[p.ydst(k)].astype(BF16)
        links.send(d2_send.at[k], d2_recv.at[k], d_ss.at[1 + k], d_rs.at[1 + k], p.tid(p.ydst(k), p.x, c))
    tree.step_y(2)
    tree.step_x(1)
    tree.step_y(3)
    tree.step_far(0)
    consume((c, 0, near), (1 - c, 0, near))
    tree.step_x(2)
    tree.step_far(1)
    consume((c, 1, near))
    tree.partner_near(1)
    column = d_own[p.y]
    for k in (1, 2, 3):
        links.wait(d2_recv.at[k], d_ss.at[1 + k], d_rs.at[1 + k], p.tid(p.ysrc(k), p.x, c))
        column = column + d2_recv[k].astype(F32)
    d3_send[...] = column.astype(BF16)
    links.send(d3_send, d3_recv, d_ss.at[5], d_rs.at[5], p.mate)
    consume((1 - c, 1, near))
    tree.step_x(3)
    tree.step_far(2)
    consume((c, 2, near), (c, 0, far))
    links.wait(d3_recv, d_ss.at[5], d_rs.at[5], p.mate)
    kvraw[c] = column + d3_recv[...].astype(F32)
    links.send(kvraw.at[c], kvraw.at[c], d_ss.at[6], d_rs.at[6], p.partner)
    tree.partner_near(2)
    tree.partner_far(0)
    consume((1 - c, 2, near), (1 - c, 0, far))
    consume((c, 3, near), (c, 1, far))
    tree.partner_near(3)
    tree.step_far(3)
    tree.partner_far(1)
    tree.partner_far(2)
    consume((1 - c, 3, near), (1 - c, 1, far))
    consume((c, 2, far), (c, 3, far), (1 - c, 2, far))
    tree.partner_far(3)
    consume((1 - c, 3, far))
    links.wait(kvraw.at[1 - c], d_ss.at[6], d_rs.at[6], p.partner)

    cosine, sine = cos_s[...], sin_s[...]
    inverse = lax.rsqrt(jnp.sum(ssq[...], axis=1, keepdims=True) * (1.0 / D) + EPSILON)

    def rotate(u):
        return u * cosine + pltpu.roll(u, HALF_DIM, 1) * (sign * sine)

    def unrotate(z, cosine, sine, sign):
        return z * cosine - pltpu.roll(z * sine, HALF_DIM, 1) * sign

    group = p.y * 2 + p.pair
    key_raw, value_raw = kvraw[0], kvraw[1]
    key = rotate(inverse * key_raw + kvbias[pl.ds(group, 1), :]).astype(BF16)
    value = (inverse * value_raw + kvbias[pl.ds(KV_HEADS + group, 1), :]).astype(BF16)
    query = jnp.concatenate(
        [rotate(inverse * acc[:, h * 128 : h * 128 + 128] + qbias[h : h + 1, :]).astype(BF16) for h in (0, 1)], axis=0
    )
    upstream = jnp.concatenate([up[:, :128], up[:, 128:]], axis=0)
    both = jnp.concatenate([allowed.astype(F32), allowed.astype(F32)], axis=0) > 0.5
    scores = jnp.where(both, mm_nt(query, key) * SCALE, -1e30)
    highest = jnp.max(scores, axis=1, keepdims=True)
    exponent = jnp.where(both, jnp.exp(scores - highest), 0.0)
    weights = exponent / jnp.sum(exponent, axis=1, keepdims=True)
    low = weights.astype(BF16)
    attended = mm(low, value).astype(BF16)
    att[:, :128] = attended[:ROWS]
    att[:, 128:] = attended[ROWS:]
    att_copy = pltpu.make_async_copy(att, att_out, local_sem.at[10])
    att_copy.start()
    weight_grad = mm_nt(upstream, value)
    inner = jnp.sum(weights * weight_grad, axis=1, keepdims=True)
    score_grad = (weights * (weight_grad - inner) * SCALE).astype(BF16)
    kv_f32[0] = mm_tn(score_grad, query)
    kv_f32[1] = mm_tn(low, upstream)
    e1_send[...] = kv_f32[...].astype(BF16)
    links.send(e1_send.at[1 - c], e1_recv, e_ss.at[0], e_rs.at[0], p.partner)
    query_grad = mm(score_grad, key)
    for h in (0, 1):
        piece = unrotate(query_grad[h * ROWS : h * ROWS + ROWS], cosine, sine, sign).astype(BF16)
        q_grad[:, h * 128 : h * 128 + 128] = piece
        product = piece.astype(F32) * acc[:, h * 128 : h * 128 + 128]
        if h == 0:
            rs_rows[pl.ds(0, ROWS), :] = product
        else:
            rs_rows[pl.ds(0, ROWS), :] += product
    rs_rows[pl.ds(ROWS, 64), :] = jnp.zeros((64, 128), F32)

    def products(k):
        rows = pl.ds(pl.multiple_of(p.ydst(k) * (8 * PART), 8 * PART), 8 * PART)
        products_s[k] = mm_nt(q_grad[...], wq[rows, :])

    def partial(k, shift, core):
        col = (lax.rem(p.x + shift, 4) * 2 + core) * PART
        return products_s[k, :, pl.ds(pl.multiple_of(col, PART), PART)]

    def f_cores(k, which=(2, 1, 3, 0)):
        for j in which:
            value = partial(k, j, 1 - c)
            if k == 0:
                value = value + kv_part[j, 1]
            f0_send[k, j] = value.astype(BF16)
            links.send(f0_send.at[k, j], f0_recv.at[k, j], c_ss.at[4 * k + j], c_rs.at[4 * k + j], p.partner)

    top, bottom = pl.ds(0, HALF), pl.ds(HALF, HALF)

    def chip_sum(k, shift):
        links.wait(f0_recv.at[k, shift], c_ss.at[4 * k + shift], c_rs.at[4 * k + shift], p.partner)
        value = partial(k, shift, c) + f0_recv[k, shift].astype(F32)
        return value + kv_part[shift, 0] if k == 0 else value

    def f_far(k):
        far_send[k] = chip_sum(k, 2).astype(BF16)
        links.send(far_send.at[k, top], far_l.at[k], f_ss.at[4 + k], f_rs.at[4 + k], p.right)
        links.send(far_send.at[k, bottom], far_r.at[k], f_ss.at[8 + k], f_rs.at[8 + k], p.left)

    def f_direct(k):
        value = chip_sum(k, 1)
        r_send[k, bottom] = value[HALF:].astype(BF16)
        links.send(r_send.at[k, bottom], from_l.at[k, bottom], f_ss.at[12 + k], f_rs.at[12 + k], p.right)
        s_r[k] = value[:HALF]
        value = chip_sum(k, 3)
        l_send[k, top] = value[:HALF].astype(BF16)
        links.send(l_send.at[k, top], from_r.at[k, top], f_ss.at[16 + k], f_rs.at[16 + k], p.left)
        s_l[k] = value[HALF:]
        s_own[k] = chip_sum(k, 0)

    def f_second(k):
        links.wait(far_l.at[k], f_ss.at[4 + k], f_rs.at[4 + k], p.left)
        r_send[k, top] = (s_r[k] + far_l[k].astype(F32)).astype(BF16)
        links.send(r_send.at[k, top], from_l.at[k, top], f_ss.at[20 + k], f_rs.at[20 + k], p.right)
        links.wait(far_r.at[k], f_ss.at[8 + k], f_rs.at[8 + k], p.right)
        l_send[k, bottom] = (s_l[k] + far_r[k].astype(F32)).astype(BF16)
        links.send(l_send.at[k, bottom], from_r.at[k, bottom], f_ss.at[24 + k], f_rs.at[24 + k], p.left)

    def f_third(k):
        links.wait(from_l.at[k, bottom], f_ss.at[12 + k], f_rs.at[12 + k], p.left)
        links.wait(from_r.at[k, top], f_ss.at[16 + k], f_rs.at[16 + k], p.right)
        links.wait(from_l.at[k, top], f_ss.at[20 + k], f_rs.at[20 + k], p.left)
        links.wait(from_r.at[k, bottom], f_ss.at[24 + k], f_rs.at[24 + k], p.right)
        value = s_own[k] + from_l[k].astype(F32) + from_r[k].astype(F32)
        if k == 0:
            s_own[k] = value
        else:
            y_send[k] = value.astype(BF16)
            links.send(
                y_send.at[k], y_recv.at[k], f_ss.at[28 + k], f_rs.at[28 + k], p.tid(p.ydst(k), p.x, c)
            )

    products(1)
    f_cores(1)
    links.wait(e1_recv, e_ss.at[0], e_rs.at[0], p.partner)
    chip_grad = kv_f32[c] + e1_recv[...].astype(F32)
    e2_send[...] = chip_grad.astype(BF16)
    links.send(e2_send, e2_recv, e_ss.at[1], e_rs.at[1], p.mate)
    products(2)
    f_far(1)
    f_cores(2)
    f_direct(1)
    f_far(2)
    links.wait(e2_recv, e_ss.at[1], e_rs.at[1], p.mate)
    value_side = c.astype(F32)
    finished = unrotate(
        kv_f32[c] + e1_recv[...].astype(F32) + e2_recv[...].astype(F32),
        cosine * (1.0 - value_side) + value_side,
        sine * (1.0 - value_side),
        sign,
    ).astype(BF16)
    rs_rows[pl.ds(0, ROWS), :] += 0.5 * finished.astype(F32) * kvraw[c]
    ones = jnp.ones((8, 128), F32)
    stat = jnp.concatenate([exact_nt(ones, rs_rows[0:128, :]), exact_nt(ones, rs_rows[128:256, :])], axis=0)
    coarse = stat.astype(BF16).astype(F32)
    ebuf[p.y, pl.ds(0, ROWS)] = finished
    ebuf[p.y, pl.ds(ROWS, 16)] = jnp.where(lax.rem(iota((16, 128), 0), 2) == 0, coarse, stat - coarse).astype(BF16)
    for k in (1, 2, 3):
        links.send(ebuf.at[p.y], ebuf.at[p.y], e_ss.at[1 + k], e_rs.at[1 + k], p.tid(p.ydst(k), p.x, c))
    f_direct(2)
    f_second(1)
    products(3)
    f_cores(3)
    f_far(3)
    f_second(2)
    products(0)
    f_cores(0, (2,))
    f_direct(3)
    f_third(1)
    f_far(0)
    f_second(3)
    for k in (1, 2, 3):
        links.wait(ebuf.at[p.ysrc(k)], e_ss.at[1 + k], e_rs.at[1 + k], p.tid(p.ysrc(k), p.x, c))
    mirror_shift = 3 - 2 * p.kind
    pair_grads = jnp.concatenate([ebuf[i, pl.ds(0, ROWS)] for i in range(4)], axis=1)
    for (tid, ref), shift, core in zip(weights_of, (0, 0, lax.rem(mirror_shift + 4, 4), lax.rem(mirror_shift + 4, 4)), (0, 1, 0, 1)):
        kv_part[shift, core] = mm_nt(pair_grads, ref[...])
    f_cores(0, (1, 3, 0))
    row_sum = jnp.zeros((16, 128), F32)
    for i in range(4):
        row_sum = row_sum + ebuf[i, pl.ds(ROWS, 16)].astype(F32)
    rs_all[p.row_index] = row_sum
    for j in range(1, 8):
        own_row = rs_all.at[p.row_index]
        links.send(own_row, own_row, r_ss.at[j], r_rs.at[j], p.in_row(j))
    f_third(2)
    f_direct(0)
    f_third(3)
    f_second(0)
    for j in range(1, 8):
        back = lax.rem(p.row_index + 8 - j, 8)
        links.wait(rs_all.at[back], r_ss.at[j], r_rs.at[j], p.y * 8 + back)
    stats = rs_all[0]
    for j in range(1, 8):
        stats = stats + rs_all[j]
    eye = iota((128, 128), 0) == iota((128, 128), 1)

    def upright(row):
        return jnp.sum(jnp.where(eye, jnp.broadcast_to(row, (128, 128)), 0.0), axis=1, keepdims=True)

    row_stat = jnp.concatenate(
        [upright(stats[0:1] + stats[1:2]), upright(stats[8:9] + stats[9:10])[: ROWS - 128]], axis=0
    ) * (1.0 / D)
    f_third(0)
    normed_grad = s_own[0]
    for k in (1, 2, 3):
        links.wait(y_recv.at[k], f_ss.at[28 + k], f_rs.at[28 + k], p.tid(p.ysrc(k), p.x, c))
        normed_grad = normed_grad + y_recv[k].astype(F32)
    own_gain = jnp.concatenate([gain[pl.ds(2 * t, 1), :], gain[pl.ds(2 * t + 1, 1), :]], axis=1)
    grad[...] = (
        inverse * (own_gain * normed_grad)
        - full[t].astype(F32) * (inverse * inverse * inverse * row_stat)
    ).astype(BF16)
    grad_copy = pltpu.make_async_copy(grad, grad_out, local_sem.at[11])
    grad_copy.start()
    lax.fori_loop(1, N_DP, drain_rollout, 0)
    links.drain()
    att_copy.wait()
    grad_copy.wait()


def hand_over(att_in, grad_in, att_out, grad_out):
    att_out[...] = att_in[...]
    grad_out[...] = grad_in[...]


def on_device(
    hidden_slots, lengths, owners, norm_gain, w_query, query_bias, w_keyvalue, keyvalue_bias, grad_attention
):
    frequency = ROPE_BASE ** (-2.0 * np.arange(HALF_DIM, dtype=np.float32) / HEAD_DIM)
    angles = np.arange(WINDOW, dtype=np.float32)[:, None] * frequency[None, :].astype(np.float32)
    angles = np.concatenate([angles, angles], axis=1)
    cosine = jnp.asarray(np.cos(angles), F32)
    sine = jnp.asarray(np.sin(angles), F32)
    operands = (
        hidden_slots, lengths, owners, norm_gain.reshape(64, 128), w_query, query_bias.reshape(2, 128),
        w_keyvalue, keyvalue_bias.reshape(16, 128), grad_attention, cosine, sine,
    )

    def v(*shape, dtype=BF16):
        return pltpu.VMEM(shape, dtype)

    def dma(n):
        return pltpu.SemaphoreType.DMA((n,))

    scratch = [pltpu.VMEM(one.shape, one.dtype) for i, one in enumerate(operands) if i != 6]
    scratch += [v(ROWS, PART), v(ROWS, PART)]
    scratch += [
        v(N_DP, WINDOW, PART), v(N_DP, WINDOW, PART), v(LANES, ROWS, PART), v(ROWS, PART, dtype=F32),
        v(ROWS, 128, dtype=F32),
    ]
    scratch += [
        v(2, 2, PART, 512), v(3, PART, 512), v(4, ROWS, 128, dtype=F32),
        v(4, ROWS, 128), v(4, ROWS, 128), v(ROWS, 128), v(ROWS, 128), v(2, ROWS, 128, dtype=F32),
    ]
    scratch += [
        v(ROWS, 128, dtype=F32), v(ROWS, 128, dtype=F32), v(ROWS, PART), v(2, ROWS, 128, dtype=F32),
        v(2, ROWS, 128), v(ROWS, 128), v(ROWS, 128), v(ROWS, 128),
        v(4, GRAD_ROWS, 128), v(256, 128, dtype=F32), v(8, 16, 128, dtype=F32), v(4, 2, ROWS, PART, dtype=F32),
        v(4, ROWS, 8 * PART, dtype=F32),
    ]
    scratch += [
        v(4, 4, ROWS, PART), v(4, 4, ROWS, PART), v(4, ROWS, PART), v(4, HALF, PART), v(4, HALF, PART),
        v(4, ROWS, PART), v(4, ROWS, PART), v(4, ROWS, PART), v(4, ROWS, PART), v(4, ROWS, PART, dtype=F32),
        v(4, HALF, PART, dtype=F32), v(4, HALF, PART, dtype=F32), v(4, ROWS, PART), v(4, ROWS, PART),
    ]
    scratch += [
        dma(28), dma(N_DP), dma(N_DP), dma(TREE_SLOTS), dma(TREE_SLOTS), dma(8), dma(8),
        dma(5), dma(5), dma(8), dma(8), dma(16), dma(16), dma(32), dma(32),
    ]
    shape = jax.ShapeDtypeStruct((ROWS, PART), BF16)
    outs = pl.pallas_call(
        kernel,
        out_shape=(shape, shape),
        in_specs=[pl.BlockSpec(memory_space=pltpu.HBM)] * len(operands),
        out_specs=[pl.BlockSpec(memory_space=pl.ANY)] * 2,
        scratch_shapes=scratch,
        compiler_params=pltpu.CompilerParams(
            collective_id=0, has_side_effects=True, vmem_limit_bytes=60 * 1024 * 1024
        ),
        name="step",
    )(*operands)
    return pl.pallas_call(hand_over, out_shape=(shape, shape), name="hand_over")(*outs)


def solution(mesh):
    in_specs = (
        P("dp", None, "tensor"),
        P(),
        P(),
        P(),
        P(None, "tensor"),
        P("tensor"),
        P("tensor", None),
        P(),
        P("dp", "tensor"),
    )
    out_specs = (P("dp", "tensor"), P("dp", "tensor"))
    return jax.shard_map(on_device, mesh=mesh, in_specs=in_specs, out_specs=out_specs, check_vma=False)
```

```python
import jax
import jax.numpy as jnp
import numpy as np
from jax import lax
from jax.experimental import pallas as pl
from jax.experimental.pallas import tpu as pltpu
from jax.sharding import PartitionSpec as P

D = 8192
HEADS = 64
KV_HEADS = 8
HEAD_DIM = 128
EPSILON = 1e-06
ROPE_BASE = 1000000.0
N_DP = 24
WINDOW = 16
ROWS = 192
HALF = 96
PART = 256
LANES = 32
HALF_DIM = HEAD_DIM // 2
SCALE = HEAD_DIM ** (-0.5)
MESH = pl.DeviceIdType.MESH
F32 = jnp.float32
BF16 = jnp.bfloat16
TREE_SLOTS = 23
GRAD_ROWS = ROWS + 16
ORDER = (1, 2, 3, 0)


def mm(a, b):
    return jnp.dot(a, b, preferred_element_type=F32)


def mm_nt(a, b):
    return lax.dot_general(a, b, (((1,), (1,)), ((), ())), preferred_element_type=F32)


def mm_tn(a, b):
    return lax.dot_general(a, b, (((0,), (0,)), ((), ())), preferred_element_type=F32)


def exact_nt(a, b):
    return lax.dot_general(
        a, b, (((1,), (1,)), ((), ())), preferred_element_type=F32, precision=lax.Precision.HIGHEST
    )


def exact_mm(a, b):
    return lax.dot_general(
        a, b, (((1,), (0,)), ((), ())), preferred_element_type=F32, precision=lax.Precision.HIGHEST
    )


def iota(shape, dim):
    return lax.broadcasted_iota(jnp.int32, shape, dim)


class Links:
    def __init__(self, dp):
        self.dp = dp

    def copy(self, src, dst, send_sem, recv_sem, peer):
        return pltpu.make_async_remote_copy(
            src_ref=src,
            dst_ref=dst,
            send_sem=send_sem,
            recv_sem=recv_sem,
            device_id=(self.dp, peer),
            device_id_type=MESH,
        )

    def send(self, src, dst, send_sem, recv_sem, peer):
        self.copy(src, dst, send_sem, recv_sem, peer).start()

    def wait(self, dst, send_sem, recv_sem, peer):
        self.copy(dst, dst, send_sem, recv_sem, peer).wait_recv()

    def sent(self, bytes_of, send_sem, recv_sem, peer):
        self.copy(bytes_of, bytes_of, send_sem, recv_sem, peer).wait_send()


class Tree:
    def __init__(self, links, place, buffer, cuts, send_sem, recv_sems, base):
        self.links = links
        self.place = place
        self.buffer = buffer
        self.small, self.large = cuts
        self.ss = send_sem
        self.rs = recv_sems
        self.base = base

    def block(self, tid):
        return self.buffer.at[tid]

    def send(self, slot, ref, peer):
        self.links.send(ref, ref, self.ss, self.rs.at[self.base + slot], peer)

    def wait(self, slot, ref, peer):
        self.links.wait(ref, self.ss, self.rs.at[self.base + slot], peer)

    def spread(self, k):
        p = self.place
        ref = self.block(p.tid(p.ysrc(k), p.x, p.c))
        self.send(3 + k, ref, p.mate)
        self.send(7 + k, ref, p.mirror)
        self.send(15 + k, ref, p.partner)

    def start(self):
        p = self.place
        ref = self.block(p.t)
        for k in (1, 2):
            self.send(k - 1, ref, p.tid(p.ydst(k), p.x, p.c))
        self.spread(0)

    def step_y(self, k):
        p = self.place
        ref = self.block(p.tid(p.ysrc(k), p.x, p.c))
        self.wait(k - 1, ref, p.tid(p.ysrc(k), p.x, p.c))
        if k == 2:
            self.send(2, ref, p.tid(p.ydst(1), p.x, p.c))
        self.spread(k)

    def step_mate(self, k):
        p = self.place
        tid = p.tid(p.ysrc(k), p.x + 1 - 2 * p.kind, p.c)
        self.wait(3 + k, self.block(tid), p.mate)
        rows = pl.ds(pl.multiple_of((1 - p.kind) * self.large, 16), self.small)
        self.send(11 + k, self.buffer.at[tid, rows], p.mirror)
        self.send(15 + k, self.block(tid), p.partner)

    def step_mirror(self, k):
        p = self.place
        tid = p.tid(p.ysrc(k), 3 - p.x, p.c)
        self.wait(7 + k, self.block(tid), p.mirror)
        rows = pl.ds(pl.multiple_of(p.kind * self.small, 16), self.large)
        self.send(11 + k, self.buffer.at[tid, rows], p.mate)
        self.send(15 + k, self.block(tid), p.partner)

    def step_far(self, k):
        p = self.place
        tid = p.tid(p.ysrc(k), p.xat(2), p.c)
        self.wait(11 + k, self.block(tid), p.left)
        self.send(19 + k, self.block(tid), p.partner)

    def partner_near(self, k):
        self.wait(15 + k, self.buffer.at[pl.ds(0, 3)], self.place.partner)

    def partner_far(self, k):
        p = self.place
        self.wait(19 + k, self.block(p.tid(p.ysrc(k), p.xat(2), 1 - p.c)), p.partner)

    def sent(self):
        self.links.sent(self.buffer.at[pl.ds(0, 31)], self.ss, self.rs.at[self.base], self.place.partner)


class Place:
    def __init__(self):
        self.dp = lax.axis_index("dp")
        self.t = lax.axis_index("tensor")
        self.c = lax.rem(self.t, 2)
        self.x = lax.rem(lax.div(self.t, 2), 4)
        self.y = lax.div(self.t, 8)
        self.left = self.tid(self.y, self.xat(3), self.c)
        self.right = self.tid(self.y, self.xat(1), self.c)
        self.partner = self.tid(self.y, self.x, 1 - self.c)
        self.pair = lax.div(self.x, 2)
        self.kind = lax.rem(self.x, 2)
        self.mirror = self.tid(self.y, 3 - self.x, self.c)
        self.mirror_other = self.tid(self.y, 3 - self.x, 1 - self.c)
        self.row_index = self.x * 2 + self.c
        self.mate = self.tid(self.y, self.x + 1 - 2 * self.kind, self.c)

    def in_row(self, j):
        return self.y * 8 + lax.rem(self.row_index + j, 8)

    def tid(self, y, x, c):
        return (y * 4 + x) * 2 + c

    def xat(self, shift):
        return lax.rem(self.x + shift, 4)

    def ydst(self, k):
        if k == 3:
            return 3 - self.y
        if k == 2:
            return self.y + 2 - 4 * lax.div(self.y, 2)
        if k == 1:
            return self.y + 1 - 2 * lax.rem(self.y, 2)
        return self.y

    def ysrc(self, k):
        return self.ydst(k)


def kernel(
    slots_in, lengths_in, owners_in, gain_in, wq_in, qbias_in, wkv_in, kvbias_in, up_in, cos_in, sin_in,
    att_out, grad_out,
    slots, lengths, owners, gain, wq, qbias, kvbias, up, cos16, sin16, att, grad,
    owner_table, a_send, a_recv, full_low, full_high, acc, ssq,
    w_own, w_far, d_own, d2_send, d2_recv, d3_send, d3_recv, kvraw,
    cos_s, sin_s, q_grad, kv_f32, e1_send, e1_recv, e2_send, e2_recv, ebuf, rs_rows, rs_all, products_s,
    f0_send, f0_recv, far_send, from_mate, from_mirror, mate_send, mirror_send, column_in, s_own, s_mate, s_mirror, y_send, y_recv,
    local_sem, a_ss, a_rs, b_ss, b_rs, d_ss, d_rs, e_ss, e_rs, f_ss, f_rs,
):
    p = Place()
    dp, t, c = p.dp, p.t, p.c

    pairs = (
        (owners_in, owner_table), (slots_in, slots), (owners_in, owners), (lengths_in, lengths), (gain_in, gain),
        (kvbias_in, kvbias), (qbias_in, qbias), (cos_in, cos16), (sin_in, sin16), (up_in, up), (wq_in, wq),
    )
    loads = [pltpu.make_async_copy(a, b, local_sem.at[i]) for i, (a, b) in enumerate(pairs)]
    weight_loads = []
    for kind in (0, 1):
        for pair in (0, 1):
            for i in range(4):
                weight_loads.append(
                    pltpu.make_async_copy(
                        wkv_in.at[:, pl.ds(kind * 1024 + (2 * i + pair) * 128, 128)],
                        w_own.at[kind, pair, :, pl.ds(i * 128, 128)],
                        local_sem.at[12],
                    )
                )
    for one in loads[:2]:
        one.start()

    barrier = pltpu.get_barrier_semaphore()

    def greet(k, carry):
        pl.semaphore_signal(barrier, inc=1, device_id=(lax.rem(dp + k, N_DP), t), device_id_type=MESH)
        return carry

    lax.fori_loop(1, N_DP, greet, 0)
    for peer in tuple(p.in_row(j) for j in range(1, 8)) + tuple(p.tid(p.ydst(k), p.x, c) for k in (1, 2, 3)):
        pl.semaphore_signal(barrier, inc=1, device_id=(dp, peer), device_id_type=MESH)

    for one in loads[2:] + weight_loads:
        one.start()

    total = N_DP * WINDOW
    loads[0].wait()
    slot_of = []
    for b in range(N_DP):
        found = jnp.int32(0)
        for j in range(1, N_DP):
            found = jnp.where(owner_table[b, j] == dp, j, found)
        slot_of.append(found)
    loads[1].wait()
    for b in range(N_DP):
        block = slots[slot_of[b]]
        for h in (0, 1):
            a_send[h, b] = block[:, h * 128 : h * 128 + 128]
    for h in (0, 1):
        a_recv[h, dp] = a_send[h, dp]
    pl.semaphore_wait(barrier, N_DP - 1 + 10)

    def rollout(src, dst, k, peer):
        return pltpu.make_async_remote_copy(
            src_ref=src, dst_ref=dst, send_sem=a_ss.at[0], recv_sem=a_rs.at[k], device_id=(peer, t), device_id_type=MESH
        )

    def send_rollout(i, carry):
        h, k = lax.div(i, N_DP - 1), lax.rem(i, N_DP - 1) + 1
        peer = lax.rem(dp + k, N_DP)
        rollout(a_send.at[h, peer], a_recv.at[h, dp], h, peer).start()
        return carry

    def wait_rollout(h):
        most = a_recv.at[h, pl.ds(0, N_DP - 1)]
        rollout(most, most, h, lax.rem(dp + 1, N_DP)).wait_recv()

    lax.fori_loop(0, 2 * (N_DP - 1), send_rollout, 0)

    pltpu.make_async_copy(w_own, w_own, local_sem.at[12]).wait()
    for one in loads[2:]:
        one.wait()
    links = Links(dp)
    links.send(w_own.at[1 - c, p.pair], w_far.at[0], d_ss.at[0], d_rs.at[0], p.partner)
    links.send(w_own.at[c, 1 - p.pair], w_far.at[1], d_ss.at[0], d_rs.at[0], p.mirror)
    links.send(w_own.at[1 - c, 1 - p.pair], w_far.at[2], d_ss.at[0], d_rs.at[0], p.mirror_other)

    length_row = jnp.broadcast_to(lengths[pl.ds(dp, 1), :].astype(F32), (ROWS, N_DP))
    owner_row = jnp.broadcast_to(owners[pl.ds(dp, 1), :].astype(F32), (ROWS, N_DP))
    before = (iota((N_DP, N_DP), 0) < iota((N_DP, N_DP), 1)).astype(F32).astype(BF16)
    starts = mm(length_row.astype(BF16), before)
    place = iota((ROWS, N_DP), 0).astype(F32)
    inside = (place >= starts) & (place < starts + length_row)
    start = jnp.sum(jnp.where(inside, starts, 0.0), axis=1, keepdims=True)
    source = jnp.sum(jnp.where(inside, owner_row, 0.0), axis=1, keepdims=True)
    offset = iota((ROWS, 1), 0).astype(F32) - start
    wanted = (source * WINDOW + offset).astype(jnp.int32)
    select = (iota((ROWS, total), 1) == wanted).astype(F32).astype(BF16)
    turn = (iota((ROWS, WINDOW), 1) == offset.astype(jnp.int32)).astype(F32)
    sign = jnp.where(iota((ROWS, HEAD_DIM), 1) < HALF_DIM, -1.0, 1.0)
    cos_s[...] = exact_mm(turn, cos16[...])
    sin_s[...] = exact_mm(turn, sin16[...])
    key_place = iota((ROWS, ROWS), 1)
    allowed = (key_place >= start.astype(jnp.int32)) & (key_place <= iota((ROWS, ROWS), 0))
    acc[...] = jnp.zeros_like(acc)
    ssq[...] = jnp.zeros_like(ssq)
    trees = [
        Tree(links, p, ref, (80, 112), b_ss.at[h], b_rs, h * TREE_SLOTS) for h, ref in enumerate((full_low, full_high))
    ]
    for h, ref in enumerate((full_low, full_high)):
        wait_rollout(h)
        ref[t] = mm(select, a_recv[h].reshape(total, 128)).astype(BF16)
        trees[h].start()

    def steps(name, k):
        for tree in trees:
            getattr(tree, name)(k)

    def scaled(tid):
        low, high = full_low[tid].astype(F32), full_high[tid].astype(F32)
        value = jnp.concatenate([low * gain[pl.ds(2 * tid, 1), :], high * gain[pl.ds(2 * tid + 1, 1), :]], axis=1)
        return value.astype(BF16), low * low + high * high

    def consume(*items):
        total, squares = None, None
        for core, k, shifts in items:
            for shift in shifts:
                tid = p.tid(p.ysrc(k), p.xat(shift), core)
                value, square = scaled(tid)
                part = mm(value, wq[pl.ds(pl.multiple_of(tid * PART, PART), PART), :])
                total = part if total is None else total + part
                squares = square if squares is None else squares + square
        ssq[...] += squares
        acc[...] += total

    near, far = (0, 1, 3), (2,)
    first, second = trees
    first.step_mate(0)
    first.step_y(1)
    first.step_mirror(0)
    first.step_y(2)
    second.step_mate(0)
    second.step_y(1)
    second.step_mirror(0)
    second.step_y(2)
    first.step_mate(1)
    first.step_y(3)
    steps("partner_near", 0)
    links.wait(w_far, d_ss.at[0], d_rs.at[0], p.partner)
    weights_of = ((t, w_own.at[c, p.pair]), (p.partner, w_far.at[0]), (p.mirror, w_far.at[1]), (p.mirror_other, w_far.at[2]))
    low_sum, high_sum = jnp.zeros((ROWS, 256), F32), jnp.zeros((ROWS, 256), F32)
    for tid, ref in weights_of:
        value = scaled(tid)[0]
        low_sum = low_sum + mm(value, ref[:, :256])
        high_sum = high_sum + mm(value, ref[:, 256:])
    for i, value in enumerate((low_sum, high_sum)):
        d_own[2 * i] = value[:, :128]
        d_own[2 * i + 1] = value[:, 128:]
    for k in (1, 2, 3):
        d2_send[k] = d_own[p.ydst(k)].astype(BF16)
        links.send(d2_send.at[k], d2_recv.at[k], d_ss.at[1], d_rs.at[1], p.tid(p.ydst(k), p.x, c))
    first.step_mirror(1)
    second.step_mate(1)
    second.step_y(3)
    second.step_mirror(1)
    steps("step_far", 0)
    consume((c, 0, near), (1 - c, 0, near))
    first.step_mate(2)
    first.step_mirror(2)
    second.step_mate(2)
    second.step_mirror(2)
    steps("step_far", 1)
    consume((c, 1, near))
    column = d_own[p.y]
    links.wait(d2_recv.at[pl.ds(1, 3)], d_ss.at[1], d_rs.at[1], p.mate)
    for k in (1, 2, 3):
        column = column + d2_recv[k].astype(F32)
    d3_send[...] = column.astype(BF16)
    links.send(d3_send, d3_recv, d_ss.at[1], d_rs.at[2], p.mate)
    steps("partner_near", 1)
    consume((1 - c, 1, near))
    steps("step_mate", 3)
    steps("step_mirror", 3)
    steps("step_far", 2)
    consume((c, 2, near), (c, 0, far))
    steps("partner_near", 2)
    steps("partner_far", 0)
    consume((1 - c, 2, near), (1 - c, 0, far))
    consume((c, 3, near))
    steps("step_far", 3)
    links.wait(d3_recv, d_ss.at[1], d_rs.at[2], p.mate)
    kvraw[c] = column + d3_recv[...].astype(F32)
    links.send(kvraw.at[c], kvraw.at[c], d_ss.at[2], d_rs.at[3], p.partner)
    consume((c, 1, far), (c, 2, far), (c, 3, far))
    steps("partner_near", 3)
    steps("partner_far", 1)
    steps("partner_far", 2)
    consume((1 - c, 3, near), (1 - c, 1, far))
    steps("partner_far", 3)
    consume((1 - c, 2, far), (1 - c, 3, far))
    links.wait(kvraw.at[1 - c], d_ss.at[2], d_rs.at[3], p.partner)

    cosine, sine = cos_s[...], sin_s[...]
    inverse = lax.rsqrt(jnp.sum(ssq[...], axis=1, keepdims=True) * (1.0 / D) + EPSILON)

    def rotate(u):
        return u * cosine + pltpu.roll(u, HALF_DIM, 1) * (sign * sine)

    def unrotate(z, cosine, sine, sign):
        return z * cosine - pltpu.roll(z * sine, HALF_DIM, 1) * sign

    group = p.y * 2 + p.pair
    key_raw, value_raw = kvraw[0], kvraw[1]
    key = rotate(inverse * key_raw + kvbias[pl.ds(group, 1), :]).astype(BF16)
    value = (inverse * value_raw + kvbias[pl.ds(KV_HEADS + group, 1), :]).astype(BF16)
    query = jnp.concatenate(
        [rotate(inverse * acc[:, h * 128 : h * 128 + 128] + qbias[h : h + 1, :]).astype(BF16) for h in (0, 1)], axis=0
    )
    upstream = jnp.concatenate([up[:, :128], up[:, 128:]], axis=0)
    both = jnp.concatenate([allowed.astype(F32), allowed.astype(F32)], axis=0) > 0.5
    scores = jnp.where(both, mm_nt(query, key) * SCALE, -1e30)
    highest = jnp.max(scores, axis=1, keepdims=True)
    exponent = jnp.where(both, jnp.exp(scores - highest), 0.0)
    weights = exponent / jnp.sum(exponent, axis=1, keepdims=True)
    low = weights.astype(BF16)
    weight_grad = mm_nt(upstream, value)
    inner = jnp.sum(weights * weight_grad, axis=1, keepdims=True)
    score_grad = (weights * (weight_grad - inner) * SCALE).astype(BF16)
    query_grad = mm(score_grad, key)
    for h in (0, 1):
        piece = unrotate(query_grad[h * ROWS : h * ROWS + ROWS], cosine, sine, sign).astype(BF16)
        q_grad[:, h * 128 : h * 128 + 128] = piece

    def products(k):
        rows = pl.ds(pl.multiple_of(p.ydst(k) * (8 * PART), 8 * PART), 8 * PART)
        products_s[k] = mm_nt(q_grad[...], wq[rows, :])

    def partial(k, shift, core):
        col = (lax.rem(p.x + shift, 4) * 2 + core) * PART
        return products_s[k, :, pl.ds(pl.multiple_of(col, PART), PART)]

    kind = p.kind
    far_shift, mate_shift, mirror_shift = 2, 1 + 2 * kind, 3 - 2 * kind

    def rows_of(index):
        return pl.ds(pl.multiple_of(index * HALF, HALF), HALF)

    def f_core(k, shift, sem, more=None):
        value = partial(k, shift, 1 - c)
        if more is not None:
            value = value + more
        f0_send[k, shift] = value.astype(BF16)
        links.send(f0_send.at[k, shift], f0_recv.at[k, shift], f_ss.at[0], f_rs.at[sem], p.partner)

    def f_cores_far(k):
        f_core(k, far_shift, k)

    def f_cores_mate(k):
        f_core(k, mate_shift, 4 + k)

    def f_cores_rest(k):
        f_core(k, mirror_shift, 8 + k)
        f_core(k, 0, 8 + k)

    def chip_sum(k, shift):
        return partial(k, shift, c) + f0_recv[k, shift].astype(F32)

    def f_far(k):
        links.wait(f0_recv.at[k, 2], f_ss.at[0], f_rs.at[k], p.partner)
        far_send[k] = chip_sum(k, far_shift).astype(BF16)
        links.send(far_send.at[k, rows_of(kind)], from_mate.at[k], f_ss.at[1], f_rs.at[12 + k], p.mate)
        links.send(far_send.at[k, rows_of(1 - kind)], from_mirror.at[k], f_ss.at[1], f_rs.at[16 + k], p.mirror)

    def f_mate(k):
        links.wait(f0_recv.at[k, 1], f_ss.at[0], f_rs.at[4 + k], p.partner)
        s_mate[k] = chip_sum(k, mate_shift)
        mate_send[k, rows_of(1 - kind)] = s_mate[k, rows_of(1 - kind)].astype(BF16)
        one = mate_send.at[k, rows_of(1 - kind)]
        links.send(one, column_in.at[k, 0, rows_of(1 - kind)], f_ss.at[1], f_rs.at[20 + k], p.mate)

    def f_rest(k, mirror_more=None, own_more=None):
        links.wait(f0_recv.at[k, pl.ds(0, 2)], f_ss.at[0], f_rs.at[8 + k], p.partner)
        value = chip_sum(k, mirror_shift)
        s_mirror[k] = value if mirror_more is None else value + mirror_more
        mirror_send[k, rows_of(kind)] = s_mirror[k, rows_of(kind)].astype(BF16)
        one = mirror_send.at[k, rows_of(kind)]
        links.send(one, column_in.at[k, 1, rows_of(kind)], f_ss.at[1], f_rs.at[20 + k], p.mirror)
        value = chip_sum(k, 0)
        s_own[k] = value if own_more is None else value + own_more

    def f_relay_mate(k):
        links.wait(from_mirror.at[k], f_ss.at[1], f_rs.at[16 + k], p.mirror)
        mate_send[k, rows_of(kind)] = (s_mate[k, rows_of(kind)] + from_mirror[k].astype(F32)).astype(BF16)
        one = mate_send.at[k, rows_of(kind)]
        links.send(one, column_in.at[k, 0, rows_of(kind)], f_ss.at[1], f_rs.at[20 + k], p.mate)

    def f_relay_mirror(k):
        links.wait(from_mate.at[k], f_ss.at[1], f_rs.at[12 + k], p.mate)
        mirror_send[k, rows_of(1 - kind)] = (s_mirror[k, rows_of(1 - kind)] + from_mate[k].astype(F32)).astype(BF16)
        one = mirror_send.at[k, rows_of(1 - kind)]
        links.send(one, column_in.at[k, 1, rows_of(1 - kind)], f_ss.at[1], f_rs.at[20 + k], p.mirror)

    def f_third(k):
        links.wait(column_in.at[k], f_ss.at[1], f_rs.at[20 + k], p.mate)
        value = s_own[k] + column_in[k, 0].astype(F32) + column_in[k, 1].astype(F32)
        if k == 0:
            s_own[k] = value
        else:
            if k == 2:
                links.wait(y_recv.at[3], f_ss.at[2], f_rs.at[26], p.tid(p.ydst(1), p.x, c))
                value = value + y_recv[3].astype(F32)
            y_send[k] = value.astype(BF16)
            peer = p.tid(p.ydst(2 if k == 2 else 1), p.x, c)
            links.send(y_send.at[k], y_recv.at[k], f_ss.at[2], f_rs.at[23 + k], peer)

    products(3)
    f_cores_far(3)
    kv_f32[0] = mm_tn(score_grad, query)
    kv_f32[1] = mm_tn(low, upstream)
    e1_send[...] = kv_f32[...].astype(BF16)
    links.send(e1_send.at[1 - c], e1_recv, e_ss.at[0], e_rs.at[0], p.partner)
    f_cores_mate(3)
    f_cores_rest(3)
    attended = mm(low, value).astype(BF16)
    att[:, :128] = attended[:ROWS]
    att[:, 128:] = attended[ROWS:]
    att_copy = pltpu.make_async_copy(att, att_out, local_sem.at[13])
    att_copy.start()
    for h in (0, 1):
        inner_part = q_grad[:, h * 128 : h * 128 + 128].astype(F32) * acc[:, h * 128 : h * 128 + 128]
        if h == 0:
            rs_rows[pl.ds(0, ROWS), :] = inner_part
        else:
            rs_rows[pl.ds(0, ROWS), :] += inner_part
    rs_rows[pl.ds(ROWS, 64), :] = jnp.zeros((64, 128), F32)
    f_far(3)
    links.wait(e1_recv, e_ss.at[0], e_rs.at[0], p.partner)
    chip_grad = kv_f32[c] + e1_recv[...].astype(F32)
    e2_send[...] = chip_grad.astype(BF16)
    links.send(e2_send, e2_recv, e_ss.at[0], e_rs.at[1], p.mate)
    f_mate(3)
    products(2)
    f_cores_far(2)
    f_cores_mate(2)
    f_cores_rest(2)
    f_rest(3)
    f_far(2)
    links.wait(e2_recv, e_ss.at[0], e_rs.at[1], p.mate)
    value_side = c.astype(F32)
    finished = unrotate(
        kv_f32[c] + e1_recv[...].astype(F32) + e2_recv[...].astype(F32),
        cosine * (1.0 - value_side) + value_side,
        sine * (1.0 - value_side),
        sign,
    ).astype(BF16)
    rs_rows[pl.ds(0, ROWS), :] += 0.5 * finished.astype(F32) * kvraw[c]
    ones = jnp.ones((8, 128), F32)
    stat = jnp.concatenate([exact_nt(ones, rs_rows[0:128, :]), exact_nt(ones, rs_rows[128:256, :])], axis=0)
    coarse = stat.astype(BF16).astype(F32)
    ebuf[p.y, pl.ds(0, ROWS)] = finished
    ebuf[p.y, pl.ds(ROWS, 16)] = jnp.where(lax.rem(iota((16, 128), 0), 2) == 0, coarse, stat - coarse).astype(BF16)
    for k in (1, 2, 3):
        links.send(ebuf.at[p.y], ebuf.at[p.y], e_ss.at[1], e_rs.at[2], p.tid(p.ydst(k), p.x, c))
    f_mate(2)
    f_rest(2)
    f_relay_mate(3)
    f_relay_mirror(3)
    products(1)
    f_cores_far(1)
    f_cores_mate(1)
    f_cores_rest(1)
    f_far(1)
    f_relay_mate(2)
    f_relay_mirror(2)
    products(0)
    f_cores_far(0)
    f_cores_mate(0)
    f_mate(1)
    f_rest(1)
    f_third(3)
    f_relay_mate(1)
    f_relay_mirror(1)
    f_far(0)
    f_mate(0)
    links.wait(ebuf.at[pl.ds(0, 3)], e_ss.at[1], e_rs.at[2], p.partner)
    pair_grads = jnp.concatenate([ebuf[i, pl.ds(0, ROWS)] for i in range(4)], axis=1)
    (_, w_me), (_, w_partner), (_, w_mirror), (_, w_mirror_other) = weights_of
    f_core(0, mirror_shift, 8, mm_nt(pair_grads, w_mirror_other[...]))
    f_core(0, 0, 8, mm_nt(pair_grads, w_partner[...]))
    row_sum = jnp.zeros((16, 128), F32)
    for i in range(4):
        row_sum = row_sum + ebuf[i, pl.ds(ROWS, 16)].astype(F32)
    rs_all[p.row_index] = row_sum
    for j in range(1, 8):
        own_row = rs_all.at[p.row_index]
        links.send(own_row, own_row, e_ss.at[2], e_rs.at[3], p.in_row(j))
    mirror_part = mm_nt(pair_grads, w_mirror[...])
    own_part = mm_nt(pair_grads, w_me[...])
    f_rest(0, mirror_part, own_part)
    f_third(2)
    f_third(1)
    f_relay_mate(0)
    f_relay_mirror(0)
    links.wait(rs_all.at[pl.ds(0, 7)], e_ss.at[2], e_rs.at[3], p.partner)
    stats = rs_all[0]
    for j in range(1, 8):
        stats = stats + rs_all[j]
    eye = iota((128, 128), 0) == iota((128, 128), 1)

    def upright(row):
        return jnp.sum(jnp.where(eye, jnp.broadcast_to(row, (128, 128)), 0.0), axis=1, keepdims=True)

    row_stat = jnp.concatenate(
        [upright(stats[0:1] + stats[1:2]), upright(stats[8:9] + stats[9:10])[: ROWS - 128]], axis=0
    ) * (1.0 / D)
    f_third(0)
    normed_grad = s_own[0]
    for k in (1, 2):
        links.wait(y_recv.at[k], f_ss.at[2], f_rs.at[23 + k], p.tid(p.ysrc(k), p.x, c))
        normed_grad = normed_grad + y_recv[k].astype(F32)
    own_gain = jnp.concatenate([gain[pl.ds(2 * t, 1), :], gain[pl.ds(2 * t + 1, 1), :]], axis=1)
    grad[...] = (
        inverse * (own_gain * normed_grad)
        - jnp.concatenate([full_low[t], full_high[t]], axis=1).astype(F32) * (inverse * inverse * inverse * row_stat)
    ).astype(BF16)
    grad_copy = pltpu.make_async_copy(grad, grad_out, local_sem.at[14])
    grad_copy.start()
    most = a_send.at[:, pl.ds(0, N_DP - 1)]
    rollout(most, most, 0, lax.rem(dp + 1, N_DP)).wait_send()
    for tree in trees:
        tree.sent()
    links.sent(w_far, d_ss.at[0], d_rs.at[0], p.partner)
    links.sent(d2_send, d_ss.at[1], d_rs.at[1], p.mate)
    links.sent(kvraw.at[c], d_ss.at[2], d_rs.at[3], p.partner)
    links.sent(e1_send, e_ss.at[0], e_rs.at[0], p.partner)
    links.sent(ebuf.at[pl.ds(0, 3)], e_ss.at[1], e_rs.at[2], p.partner)
    links.sent(rs_all.at[pl.ds(0, 7)], e_ss.at[2], e_rs.at[3], p.partner)
    links.sent(f0_send, f_ss.at[0], f_rs.at[0], p.partner)
    links.sent(f0_send.at[pl.ds(0, 3)], f_ss.at[1], f_rs.at[0], p.partner)
    links.sent(y_send.at[pl.ds(0, 3)], f_ss.at[2], f_rs.at[0], p.partner)
    att_copy.wait()
    grad_copy.wait()


def hand_over(att_in, grad_in, att_out, grad_out):
    att_out[...] = att_in[...]
    grad_out[...] = grad_in[...]


def on_device(
    hidden_slots, lengths, owners, norm_gain, w_query, query_bias, w_keyvalue, keyvalue_bias, grad_attention
):
    frequency = ROPE_BASE ** (-2.0 * np.arange(HALF_DIM, dtype=np.float32) / HEAD_DIM)
    angles = np.arange(WINDOW, dtype=np.float32)[:, None] * frequency[None, :].astype(np.float32)
    angles = np.concatenate([angles, angles], axis=1)
    cosine = jnp.asarray(np.cos(angles), F32)
    sine = jnp.asarray(np.sin(angles), F32)
    operands = (
        hidden_slots, lengths, owners, norm_gain.reshape(64, 128), w_query, query_bias.reshape(2, 128),
        w_keyvalue, keyvalue_bias.reshape(16, 128), grad_attention, cosine, sine,
    )

    def v(*shape, dtype=BF16):
        return pltpu.VMEM(shape, dtype)

    def dma(n):
        return pltpu.SemaphoreType.DMA((n,))

    scratch = [pltpu.VMEM(one.shape, one.dtype) for i, one in enumerate(operands) if i != 6]
    scratch += [v(ROWS, PART), v(ROWS, PART)]
    scratch += [
        pltpu.SMEM((N_DP, N_DP), jnp.int32), v(2, N_DP, WINDOW, 128), v(2, N_DP, WINDOW, 128), v(LANES, ROWS, 128),
        v(LANES, ROWS, 128), v(ROWS, PART, dtype=F32),
        v(ROWS, 128, dtype=F32),
    ]
    scratch += [
        v(2, 2, PART, 512), v(3, PART, 512), v(4, ROWS, 128, dtype=F32),
        v(4, ROWS, 128), v(4, ROWS, 128), v(ROWS, 128), v(ROWS, 128), v(2, ROWS, 128, dtype=F32),
    ]
    scratch += [
        v(ROWS, 128, dtype=F32), v(ROWS, 128, dtype=F32), v(ROWS, PART), v(2, ROWS, 128, dtype=F32),
        v(2, ROWS, 128), v(ROWS, 128), v(ROWS, 128), v(ROWS, 128),
        v(4, GRAD_ROWS, 128), v(256, 128, dtype=F32), v(8, 16, 128, dtype=F32),
        v(4, ROWS, 8 * PART, dtype=F32),
    ]
    scratch += [
        v(4, 4, ROWS, PART), v(4, 4, ROWS, PART), v(4, ROWS, PART), v(4, HALF, PART), v(4, HALF, PART),
        v(4, ROWS, PART), v(4, ROWS, PART), v(4, 2, ROWS, PART), v(4, ROWS, PART, dtype=F32),
        v(4, ROWS, PART, dtype=F32), v(4, ROWS, PART, dtype=F32), v(4, ROWS, PART), v(4, ROWS, PART),
    ]
    scratch += [
        dma(15), dma(1), dma(2), dma(2), dma(2 * TREE_SLOTS), dma(3), dma(4), dma(3), dma(4), dma(3), dma(27),
    ]
    shape = jax.ShapeDtypeStruct((ROWS, PART), BF16)
    outs = pl.pallas_call(
        kernel,
        out_shape=(shape, shape),
        in_specs=[pl.BlockSpec(memory_space=pltpu.HBM)] * len(operands),
        out_specs=[pl.BlockSpec(memory_space=pl.ANY)] * 2,
        scratch_shapes=scratch,
        compiler_params=pltpu.CompilerParams(
            collective_id=0, has_side_effects=True, vmem_limit_bytes=60 * 1024 * 1024
        ),
        name="step",
    )(*operands)
    return pl.pallas_call(hand_over, out_shape=(shape, shape), name="hand_over")(*outs)


def solution(mesh):
    in_specs = (
        P("dp", None, "tensor"),
        P(),
        P(),
        P(),
        P(None, "tensor"),
        P("tensor"),
        P("tensor", None),
        P(),
        P("dp", "tensor"),
    )
    out_specs = (P("dp", "tensor"), P("dp", "tensor"))
    return jax.shard_map(on_device, mesh=mesh, in_specs=in_specs, out_specs=out_specs, check_vma=False)
```

```python
import jax
import jax.numpy as jnp
import numpy as np
from jax import lax
from jax.experimental import pallas as pl
from jax.experimental.pallas import tpu as pltpu
from jax.sharding import PartitionSpec as P

D = 8192
HEADS = 64
KV_HEADS = 8
HEAD_DIM = 128
EPSILON = 1e-06
ROPE_BASE = 1000000.0
N_DP = 24
WINDOW = 16
ROWS = 192
HALF = 96
PART = 256
LANES = 32
HALF_DIM = HEAD_DIM // 2
SCALE = HEAD_DIM ** (-0.5)
MESH = pl.DeviceIdType.MESH
F32 = jnp.float32
BF16 = jnp.bfloat16
TREE_SLOTS = 23
GRAD_ROWS = ROWS + 16
ORDER = (1, 2, 3, 0)


def mm(a, b):
    return jnp.dot(a, b, preferred_element_type=F32)


def mm_nt(a, b):
    return lax.dot_general(a, b, (((1,), (1,)), ((), ())), preferred_element_type=F32)


def mm_tn(a, b):
    return lax.dot_general(a, b, (((0,), (0,)), ((), ())), preferred_element_type=F32)


def exact_nt(a, b):
    return lax.dot_general(
        a, b, (((1,), (1,)), ((), ())), preferred_element_type=F32, precision=lax.Precision.HIGHEST
    )


def exact_mm(a, b):
    return lax.dot_general(
        a, b, (((1,), (0,)), ((), ())), preferred_element_type=F32, precision=lax.Precision.HIGHEST
    )


def iota(shape, dim):
    return lax.broadcasted_iota(jnp.int32, shape, dim)


class Links:
    def __init__(self, dp):
        self.dp = dp

    def copy(self, src, dst, send_sem, recv_sem, peer):
        return pltpu.make_async_remote_copy(
            src_ref=src,
            dst_ref=dst,
            send_sem=send_sem,
            recv_sem=recv_sem,
            device_id=(self.dp, peer),
            device_id_type=MESH,
        )

    def send(self, src, dst, send_sem, recv_sem, peer):
        self.copy(src, dst, send_sem, recv_sem, peer).start()

    def wait(self, dst, send_sem, recv_sem, peer):
        self.copy(dst, dst, send_sem, recv_sem, peer).wait_recv()

    def sent(self, bytes_of, send_sem, recv_sem, peer):
        self.copy(bytes_of, bytes_of, send_sem, recv_sem, peer).wait_send()


class Tree:
    def __init__(self, links, place, buffer, cuts, send_sem, recv_sems, base):
        self.links = links
        self.place = place
        self.buffer = buffer
        self.small, self.large = cuts
        self.ss = send_sem
        self.rs = recv_sems
        self.base = base

    def block(self, tid):
        return self.buffer.at[tid]

    def send(self, slot, ref, peer):
        self.links.send(ref, ref, self.ss, self.rs.at[self.base + slot], peer)

    def wait(self, slot, ref, peer):
        self.links.wait(ref, self.ss, self.rs.at[self.base + slot], peer)

    def spread(self, k):
        p = self.place
        ref = self.block(p.tid(p.ysrc(k), p.x, p.c))
        self.send(3 + k, ref, p.mate)
        self.send(7 + k, ref, p.mirror)
        self.send(15 + k, ref, p.partner)

    def start(self):
        p = self.place
        ref = self.block(p.t)
        for k in (1, 2):
            self.send(k - 1, ref, p.tid(p.ydst(k), p.x, p.c))
        self.spread(0)

    def step_y(self, k):
        p = self.place
        ref = self.block(p.tid(p.ysrc(k), p.x, p.c))
        self.wait(k - 1, ref, p.tid(p.ysrc(k), p.x, p.c))
        if k == 2:
            self.send(2, ref, p.tid(p.ydst(1), p.x, p.c))
        self.spread(k)

    def step_mate(self, k):
        p = self.place
        tid = p.tid(p.ysrc(k), p.x + 1 - 2 * p.kind, p.c)
        self.wait(3 + k, self.block(tid), p.mate)
        rows = pl.ds(pl.multiple_of((1 - p.kind) * self.large, 16), self.small)
        self.send(11 + k, self.buffer.at[tid, rows], p.mirror)
        self.send(15 + k, self.block(tid), p.partner)

    def step_mirror(self, k):
        p = self.place
        tid = p.tid(p.ysrc(k), 3 - p.x, p.c)
        self.wait(7 + k, self.block(tid), p.mirror)
        rows = pl.ds(pl.multiple_of(p.kind * self.small, 16), self.large)
        self.send(11 + k, self.buffer.at[tid, rows], p.mate)
        self.send(15 + k, self.block(tid), p.partner)

    def step_far(self, k):
        p = self.place
        tid = p.tid(p.ysrc(k), p.xat(2), p.c)
        self.wait(11 + k, self.block(tid), p.left)
        self.send(19 + k, self.block(tid), p.partner)

    def partner_near(self, k):
        self.wait(15 + k, self.buffer.at[pl.ds(0, 3)], self.place.partner)

    def partner_far(self, k):
        p = self.place
        self.wait(19 + k, self.block(p.tid(p.ysrc(k), p.xat(2), 1 - p.c)), p.partner)

    def sent(self):
        self.links.sent(self.buffer.at[pl.ds(0, 31)], self.ss, self.rs.at[self.base], self.place.partner)


class Place:
    def __init__(self):
        self.dp = lax.axis_index("dp")
        self.t = lax.axis_index("tensor")
        self.c = lax.rem(self.t, 2)
        self.x = lax.rem(lax.div(self.t, 2), 4)
        self.y = lax.div(self.t, 8)
        self.left = self.tid(self.y, self.xat(3), self.c)
        self.right = self.tid(self.y, self.xat(1), self.c)
        self.partner = self.tid(self.y, self.x, 1 - self.c)
        self.pair = lax.div(self.x, 2)
        self.kind = lax.rem(self.x, 2)
        self.mirror = self.tid(self.y, 3 - self.x, self.c)
        self.mirror_other = self.tid(self.y, 3 - self.x, 1 - self.c)
        self.row_index = self.x * 2 + self.c
        self.mate = self.tid(self.y, self.x + 1 - 2 * self.kind, self.c)

    def in_row(self, j):
        return self.y * 8 + lax.rem(self.row_index + j, 8)

    def tid(self, y, x, c):
        return (y * 4 + x) * 2 + c

    def xat(self, shift):
        return lax.rem(self.x + shift, 4)

    def ydst(self, k):
        if k == 3:
            return 3 - self.y
        if k == 2:
            return self.y + 2 - 4 * lax.div(self.y, 2)
        if k == 1:
            return self.y + 1 - 2 * lax.rem(self.y, 2)
        return self.y

    def ysrc(self, k):
        return self.ydst(k)


def kernel(
    slots_in, lengths_in, owners_in, gain_in, wq_in, qbias_in, wkv_in, kvbias_in, up_in, cos_in, sin_in,
    att_out, grad_out,
    slots, lengths, owners, gain, wq, qbias, kvbias, up, cos16, sin16, att, grad,
    owner_table, a_send, a_recv, full_low, full_high, acc, ssq,
    w_own, w_far, d_own, d2_send, d2_recv, d3_send, d3_recv, kvraw,
    cos_s, sin_s, q_grad, kv_f32, e1_send, e1_recv, e2_send, e2_recv, ebuf, rs_rows, rs_all, products_s,
    f0_send, f0_recv, far_send, from_mate, from_mirror, mate_send, mirror_send, column_in, s_own, s_mate, s_mirror, y_send, y_recv,
    local_sem, a_ss, a_rs, b_ss, b_rs, d_ss, d_rs, e_ss, e_rs, f_ss, f_rs,
):
    p = Place()
    dp, t, c = p.dp, p.t, p.c

    pairs = (
        (owners_in, owner_table), (slots_in, slots), (owners_in, owners), (lengths_in, lengths), (gain_in, gain),
        (kvbias_in, kvbias), (qbias_in, qbias), (cos_in, cos16), (sin_in, sin16), (up_in, up), (wq_in, wq),
    )
    loads = [pltpu.make_async_copy(a, b, local_sem.at[i]) for i, (a, b) in enumerate(pairs)]
    weight_loads = []
    for kind in (0, 1):
        for pair in (0, 1):
            for i in range(4):
                weight_loads.append(
                    pltpu.make_async_copy(
                        wkv_in.at[:, pl.ds(kind * 1024 + (2 * i + pair) * 128, 128)],
                        w_own.at[kind, pair, :, pl.ds(i * 128, 128)],
                        local_sem.at[12],
                    )
                )
    for one in loads[:2]:
        one.start()

    barrier = pltpu.get_barrier_semaphore()

    half_index, depth = lax.div(dp, 12), lax.rem(dp, 12)
    offsets = [(dh, dz) for dh in (0, 1) for dz in range(12) if dh or dz]
    offsets.sort(key=lambda o: -(4 * o[0] + min(o[1], 12 - o[1])))
    batch_peers = [lax.rem(half_index + dh, 2) * 12 + lax.rem(depth + dz, 12) for dh, dz in offsets]
    for peer in batch_peers:
        pl.semaphore_signal(barrier, inc=1, device_id=(peer, t), device_id_type=MESH)
    for peer in tuple(p.in_row(j) for j in range(1, 8)) + tuple(p.tid(p.ydst(k), p.x, c) for k in (1, 2, 3)):
        pl.semaphore_signal(barrier, inc=1, device_id=(dp, peer), device_id_type=MESH)

    for one in loads[2:] + weight_loads:
        one.start()

    total = N_DP * WINDOW
    loads[0].wait()
    slot_of = []
    for b in range(N_DP):
        found = jnp.int32(0)
        for j in range(1, N_DP):
            found = jnp.where(owner_table[b, j] == dp, j, found)
        slot_of.append(found)
    loads[1].wait()
    for b in range(N_DP):
        block = slots[slot_of[b]]
        for h in (0, 1):
            a_send[h, b] = block[:, h * 128 : h * 128 + 128]
    for h in (0, 1):
        a_recv[h, dp] = a_send[h, dp]
    pl.semaphore_wait(barrier, N_DP - 1 + 10)

    def rollout(src, dst, k, peer):
        return pltpu.make_async_remote_copy(
            src_ref=src, dst_ref=dst, send_sem=a_ss.at[0], recv_sem=a_rs.at[k], device_id=(peer, t), device_id_type=MESH
        )

    def wait_rollout(h):
        most = a_recv.at[h, pl.ds(0, N_DP - 1)]
        rollout(most, most, h, lax.rem(dp + 1, N_DP)).wait_recv()

    for h in (0, 1):
        for peer in batch_peers:
            rollout(a_send.at[h, peer], a_recv.at[h, dp], h, peer).start()

    pltpu.make_async_copy(w_own, w_own, local_sem.at[12]).wait()
    for one in loads[2:]:
        one.wait()
    links = Links(dp)
    links.send(w_own.at[1 - c, p.pair], w_far.at[0], d_ss.at[0], d_rs.at[0], p.partner)
    links.send(w_own.at[c, 1 - p.pair], w_far.at[1], d_ss.at[0], d_rs.at[0], p.mirror)
    links.send(w_own.at[1 - c, 1 - p.pair], w_far.at[2], d_ss.at[0], d_rs.at[0], p.mirror_other)

    length_row = jnp.broadcast_to(lengths[pl.ds(dp, 1), :].astype(F32), (ROWS, N_DP))
    owner_row = jnp.broadcast_to(owners[pl.ds(dp, 1), :].astype(F32), (ROWS, N_DP))
    before = (iota((N_DP, N_DP), 0) < iota((N_DP, N_DP), 1)).astype(F32).astype(BF16)
    starts = mm(length_row.astype(BF16), before)
    place = iota((ROWS, N_DP), 0).astype(F32)
    inside = (place >= starts) & (place < starts + length_row)
    start = jnp.sum(jnp.where(inside, starts, 0.0), axis=1, keepdims=True)
    source = jnp.sum(jnp.where(inside, owner_row, 0.0), axis=1, keepdims=True)
    offset = iota((ROWS, 1), 0).astype(F32) - start
    wanted = (source * WINDOW + offset).astype(jnp.int32)
    select = (iota((ROWS, total), 1) == wanted).astype(F32).astype(BF16)
    turn = (iota((ROWS, WINDOW), 1) == offset.astype(jnp.int32)).astype(F32)
    sign = jnp.where(iota((ROWS, HEAD_DIM), 1) < HALF_DIM, -1.0, 1.0)
    cos_s[...] = exact_mm(turn, cos16[...])
    sin_s[...] = exact_mm(turn, sin16[...])
    key_place = iota((ROWS, ROWS), 1)
    allowed = (key_place >= start.astype(jnp.int32)) & (key_place <= iota((ROWS, ROWS), 0))
    acc[...] = jnp.zeros_like(acc)
    ssq[...] = jnp.zeros_like(ssq)
    trees = [
        Tree(links, p, ref, (80, 112), b_ss.at[h], b_rs, h * TREE_SLOTS) for h, ref in enumerate((full_low, full_high))
    ]
    for h, ref in enumerate((full_low, full_high)):
        wait_rollout(h)
        ref[t] = mm(select, a_recv[h].reshape(total, 128)).astype(BF16)
        trees[h].start()

    def steps(name, k):
        for tree in trees:
            getattr(tree, name)(k)

    def scaled(tid):
        low, high = full_low[tid].astype(F32), full_high[tid].astype(F32)
        value = jnp.concatenate([low * gain[pl.ds(2 * tid, 1), :], high * gain[pl.ds(2 * tid + 1, 1), :]], axis=1)
        return value.astype(BF16), low * low + high * high

    def consume(*items):
        total, squares = None, None
        for core, k, shifts in items:
            for shift in shifts:
                tid = p.tid(p.ysrc(k), p.xat(shift), core)
                value, square = scaled(tid)
                part = mm(value, wq[pl.ds(pl.multiple_of(tid * PART, PART), PART), :])
                total = part if total is None else total + part
                squares = square if squares is None else squares + square
        ssq[...] += squares
        acc[...] += total

    near, far = (0, 1, 3), (2,)
    first, second = trees
    first.step_mate(0)
    first.step_y(1)
    first.step_mirror(0)
    first.step_y(2)
    second.step_mate(0)
    second.step_y(1)
    second.step_mirror(0)
    second.step_y(2)
    first.step_mate(1)
    first.step_y(3)
    steps("partner_near", 0)
    links.wait(w_far, d_ss.at[0], d_rs.at[0], p.partner)
    weights_of = ((t, w_own.at[c, p.pair]), (p.partner, w_far.at[0]), (p.mirror, w_far.at[1]), (p.mirror_other, w_far.at[2]))
    low_sum, high_sum = jnp.zeros((ROWS, 256), F32), jnp.zeros((ROWS, 256), F32)
    for tid, ref in weights_of:
        value = scaled(tid)[0]
        low_sum = low_sum + mm(value, ref[:, :256])
        high_sum = high_sum + mm(value, ref[:, 256:])
    for i, value in enumerate((low_sum, high_sum)):
        d_own[2 * i] = value[:, :128]
        d_own[2 * i + 1] = value[:, 128:]
    for k in (1, 2, 3):
        d2_send[k] = d_own[p.ydst(k)].astype(BF16)
        links.send(d2_send.at[k], d2_recv.at[k], d_ss.at[1], d_rs.at[1], p.tid(p.ydst(k), p.x, c))
    first.step_mirror(1)
    second.step_mate(1)
    second.step_y(3)
    second.step_mirror(1)
    steps("step_far", 0)
    consume((c, 0, near), (1 - c, 0, near))
    first.step_mate(2)
    first.step_mirror(2)
    second.step_mate(2)
    second.step_mirror(2)
    steps("step_far", 1)
    consume((c, 1, near))
    column = d_own[p.y]
    links.wait(d2_recv.at[pl.ds(1, 3)], d_ss.at[1], d_rs.at[1], p.mate)
    for k in (1, 2, 3):
        column = column + d2_recv[k].astype(F32)
    d3_send[...] = column.astype(BF16)
    links.send(d3_send, d3_recv, d_ss.at[1], d_rs.at[2], p.mate)
    steps("partner_near", 1)
    consume((1 - c, 1, near))
    steps("step_mate", 3)
    steps("step_mirror", 3)
    steps("step_far", 2)
    consume((c, 2, near), (c, 0, far))
    steps("partner_near", 2)
    steps("partner_far", 0)
    consume((1 - c, 2, near), (1 - c, 0, far))
    consume((c, 3, near))
    steps("step_far", 3)
    links.wait(d3_recv, d_ss.at[1], d_rs.at[2], p.mate)
    kvraw[c] = column + d3_recv[...].astype(F32)
    links.send(kvraw.at[c], kvraw.at[c], d_ss.at[2], d_rs.at[3], p.partner)
    consume((c, 1, far), (c, 2, far), (c, 3, far))
    steps("partner_near", 3)
    steps("partner_far", 1)
    steps("partner_far", 2)
    consume((1 - c, 3, near), (1 - c, 1, far))
    steps("partner_far", 3)
    consume((1 - c, 2, far), (1 - c, 3, far))
    links.wait(kvraw.at[1 - c], d_ss.at[2], d_rs.at[3], p.partner)

    cosine, sine = cos_s[...], sin_s[...]
    inverse = lax.rsqrt(jnp.sum(ssq[...], axis=1, keepdims=True) * (1.0 / D) + EPSILON)

    def rotate(u):
        return u * cosine + pltpu.roll(u, HALF_DIM, 1) * (sign * sine)

    def unrotate(z, cosine, sine, sign):
        return z * cosine - pltpu.roll(z * sine, HALF_DIM, 1) * sign

    group = p.y * 2 + p.pair
    key_raw, value_raw = kvraw[0], kvraw[1]
    key = rotate(inverse * key_raw + kvbias[pl.ds(group, 1), :]).astype(BF16)
    value = (inverse * value_raw + kvbias[pl.ds(KV_HEADS + group, 1), :]).astype(BF16)
    query = jnp.concatenate(
        [rotate(inverse * acc[:, h * 128 : h * 128 + 128] + qbias[h : h + 1, :]).astype(BF16) for h in (0, 1)], axis=0
    )
    upstream = jnp.concatenate([up[:, :128], up[:, 128:]], axis=0)
    both = jnp.concatenate([allowed.astype(F32), allowed.astype(F32)], axis=0) > 0.5
    scores = jnp.where(both, mm_nt(query, key) * SCALE, -1e30)
    highest = jnp.max(scores, axis=1, keepdims=True)
    exponent = jnp.where(both, jnp.exp(scores - highest), 0.0)
    weights = exponent / jnp.sum(exponent, axis=1, keepdims=True)
    low = weights.astype(BF16)
    weight_grad = mm_nt(upstream, value)
    inner = jnp.sum(weights * weight_grad, axis=1, keepdims=True)
    score_grad = (weights * (weight_grad - inner) * SCALE).astype(BF16)
    query_grad = mm(score_grad, key)
    for h in (0, 1):
        piece = unrotate(query_grad[h * ROWS : h * ROWS + ROWS], cosine, sine, sign).astype(BF16)
        q_grad[:, h * 128 : h * 128 + 128] = piece

    def products(k):
        rows = pl.ds(pl.multiple_of(p.ydst(k) * (8 * PART), 8 * PART), 8 * PART)
        products_s[k] = mm_nt(q_grad[...], wq[rows, :])

    def partial(k, shift, core):
        col = (lax.rem(p.x + shift, 4) * 2 + core) * PART
        return products_s[k, :, pl.ds(pl.multiple_of(col, PART), PART)]

    kind = p.kind
    far_shift, mate_shift, mirror_shift = 2, 1 + 2 * kind, 3 - 2 * kind

    def rows_of(index):
        return pl.ds(pl.multiple_of(index * HALF, HALF), HALF)

    def f_core(k, shift, sem, more=None):
        value = partial(k, shift, 1 - c)
        if more is not None:
            value = value + more
        f0_send[k, shift] = value.astype(BF16)
        links.send(f0_send.at[k, shift], f0_recv.at[k, shift], f_ss.at[0], f_rs.at[sem], p.partner)

    def f_cores_far(k):
        f_core(k, far_shift, k)

    def f_cores_mate(k):
        f_core(k, mate_shift, 4 + k)

    def f_cores_rest(k):
        f_core(k, mirror_shift, 8 + k)
        f_core(k, 0, 8 + k)

    def chip_sum(k, shift):
        return partial(k, shift, c) + f0_recv[k, shift].astype(F32)

    def f_far(k):
        links.wait(f0_recv.at[k, 2], f_ss.at[0], f_rs.at[k], p.partner)
        far_send[k] = chip_sum(k, far_shift).astype(BF16)
        links.send(far_send.at[k, rows_of(kind)], from_mate.at[k], f_ss.at[1], f_rs.at[12 + k], p.mate)
        links.send(far_send.at[k, rows_of(1 - kind)], from_mirror.at[k], f_ss.at[1], f_rs.at[16 + k], p.mirror)

    def f_mate(k):
        links.wait(f0_recv.at[k, 1], f_ss.at[0], f_rs.at[4 + k], p.partner)
        s_mate[k] = chip_sum(k, mate_shift)
        mate_send[k, rows_of(1 - kind)] = s_mate[k, rows_of(1 - kind)].astype(BF16)
        one = mate_send.at[k, rows_of(1 - kind)]
        links.send(one, column_in.at[k, 0, rows_of(1 - kind)], f_ss.at[1], f_rs.at[20 + k], p.mate)

    def f_rest(k, mirror_more=None, own_more=None):
        links.wait(f0_recv.at[k, pl.ds(0, 2)], f_ss.at[0], f_rs.at[8 + k], p.partner)
        value = chip_sum(k, mirror_shift)
        s_mirror[k] = value if mirror_more is None else value + mirror_more
        mirror_send[k, rows_of(kind)] = s_mirror[k, rows_of(kind)].astype(BF16)
        one = mirror_send.at[k, rows_of(kind)]
        links.send(one, column_in.at[k, 1, rows_of(kind)], f_ss.at[1], f_rs.at[20 + k], p.mirror)
        value = chip_sum(k, 0)
        s_own[k] = value if own_more is None else value + own_more

    def f_relay_mate(k):
        links.wait(from_mirror.at[k], f_ss.at[1], f_rs.at[16 + k], p.mirror)
        mate_send[k, rows_of(kind)] = (s_mate[k, rows_of(kind)] + from_mirror[k].astype(F32)).astype(BF16)
        one = mate_send.at[k, rows_of(kind)]
        links.send(one, column_in.at[k, 0, rows_of(kind)], f_ss.at[1], f_rs.at[20 + k], p.mate)

    def f_relay_mirror(k):
        links.wait(from_mate.at[k], f_ss.at[1], f_rs.at[12 + k], p.mate)
        mirror_send[k, rows_of(1 - kind)] = (s_mirror[k, rows_of(1 - kind)] + from_mate[k].astype(F32)).astype(BF16)
        one = mirror_send.at[k, rows_of(1 - kind)]
        links.send(one, column_in.at[k, 1, rows_of(1 - kind)], f_ss.at[1], f_rs.at[20 + k], p.mirror)

    def f_third(k):
        links.wait(column_in.at[k], f_ss.at[1], f_rs.at[20 + k], p.mate)
        value = s_own[k] + column_in[k, 0].astype(F32) + column_in[k, 1].astype(F32)
        if k == 0:
            s_own[k] = value
        else:
            if k == 2:
                links.wait(y_recv.at[3], f_ss.at[2], f_rs.at[26], p.tid(p.ydst(1), p.x, c))
                value = value + y_recv[3].astype(F32)
            y_send[k] = value.astype(BF16)
            peer = p.tid(p.ydst(2 if k == 2 else 1), p.x, c)
            links.send(y_send.at[k], y_recv.at[k], f_ss.at[2], f_rs.at[23 + k], peer)

    far_tid = p.tid(p.ydst(3), p.xat(2), 1 - c)
    far_rows = pl.ds(pl.multiple_of(far_tid * PART, PART), PART)
    f0_send[3, 2] = mm_nt(q_grad[...], wq[far_rows, :]).astype(BF16)
    links.send(f0_send.at[3, 2], f0_recv.at[3, 2], f_ss.at[0], f_rs.at[3], p.partner)
    products(3)
    kv_f32[0] = mm_tn(score_grad, query)
    kv_f32[1] = mm_tn(low, upstream)
    e1_send[...] = kv_f32[...].astype(BF16)
    links.send(e1_send.at[1 - c], e1_recv, e_ss.at[0], e_rs.at[0], p.partner)
    f_cores_mate(3)
    f_cores_rest(3)
    attended = mm(low, value).astype(BF16)
    att[:, :128] = attended[:ROWS]
    att[:, 128:] = attended[ROWS:]
    att_copy = pltpu.make_async_copy(att, att_out, local_sem.at[13])
    att_copy.start()
    for h in (0, 1):
        inner_part = q_grad[:, h * 128 : h * 128 + 128].astype(F32) * acc[:, h * 128 : h * 128 + 128]
        if h == 0:
            rs_rows[pl.ds(0, ROWS), :] = inner_part
        else:
            rs_rows[pl.ds(0, ROWS), :] += inner_part
    rs_rows[pl.ds(ROWS, 64), :] = jnp.zeros((64, 128), F32)
    f_far(3)
    links.wait(e1_recv, e_ss.at[0], e_rs.at[0], p.partner)
    chip_grad = kv_f32[c] + e1_recv[...].astype(F32)
    e2_send[...] = chip_grad.astype(BF16)
    links.send(e2_send, e2_recv, e_ss.at[0], e_rs.at[1], p.mate)
    f_mate(3)
    products(2)
    f_cores_far(2)
    f_cores_mate(2)
    f_cores_rest(2)
    f_rest(3)
    f_far(2)
    f_mate(2)
    f_rest(2)
    f_relay_mate(3)
    f_relay_mirror(3)
    links.wait(e2_recv, e_ss.at[0], e_rs.at[1], p.mate)
    value_side = c.astype(F32)
    finished = unrotate(
        kv_f32[c] + e1_recv[...].astype(F32) + e2_recv[...].astype(F32),
        cosine * (1.0 - value_side) + value_side,
        sine * (1.0 - value_side),
        sign,
    ).astype(BF16)
    rs_rows[pl.ds(0, ROWS), :] += 0.5 * finished.astype(F32) * kvraw[c]
    ones = jnp.ones((8, 128), F32)
    stat = jnp.concatenate([exact_nt(ones, rs_rows[0:128, :]), exact_nt(ones, rs_rows[128:256, :])], axis=0)
    coarse = stat.astype(BF16).astype(F32)
    ebuf[p.y, pl.ds(0, ROWS)] = finished
    ebuf[p.y, pl.ds(ROWS, 16)] = jnp.where(lax.rem(iota((16, 128), 0), 2) == 0, coarse, stat - coarse).astype(BF16)
    for k in (1, 2, 3):
        links.send(ebuf.at[p.y], ebuf.at[p.y], e_ss.at[1], e_rs.at[2], p.tid(p.ydst(k), p.x, c))
    products(1)
    f_cores_far(1)
    f_cores_mate(1)
    f_cores_rest(1)
    f_far(1)
    f_relay_mate(2)
    f_relay_mirror(2)
    products(0)
    f_cores_far(0)
    f_cores_mate(0)
    f_mate(1)
    f_rest(1)
    f_third(3)
    f_relay_mate(1)
    f_relay_mirror(1)
    f_far(0)
    f_mate(0)
    links.wait(ebuf.at[pl.ds(0, 3)], e_ss.at[1], e_rs.at[2], p.partner)
    pair_grads = jnp.concatenate([ebuf[i, pl.ds(0, ROWS)] for i in range(4)], axis=1)
    (_, w_me), (_, w_partner), (_, w_mirror), (_, w_mirror_other) = weights_of
    f_core(0, mirror_shift, 8, mm_nt(pair_grads, w_mirror_other[...]))
    f_core(0, 0, 8, mm_nt(pair_grads, w_partner[...]))
    row_sum = jnp.zeros((16, 128), F32)
    for i in range(4):
        row_sum = row_sum + ebuf[i, pl.ds(ROWS, 16)].astype(F32)
    rs_all[p.row_index] = row_sum
    for j in range(1, 8):
        own_row = rs_all.at[p.row_index]
        links.send(own_row, own_row, e_ss.at[2], e_rs.at[3], p.in_row(j))
    mirror_part = mm_nt(pair_grads, w_mirror[...])
    own_part = mm_nt(pair_grads, w_me[...])
    f_rest(0, mirror_part, own_part)
    f_third(2)
    f_third(1)
    f_relay_mate(0)
    f_relay_mirror(0)
    links.wait(rs_all.at[pl.ds(0, 7)], e_ss.at[2], e_rs.at[3], p.partner)
    stats = rs_all[0]
    for j in range(1, 8):
        stats = stats + rs_all[j]
    eye = iota((128, 128), 0) == iota((128, 128), 1)

    def upright(row):
        return jnp.sum(jnp.where(eye, jnp.broadcast_to(row, (128, 128)), 0.0), axis=1, keepdims=True)

    row_stat = jnp.concatenate(
        [upright(stats[0:1] + stats[1:2]), upright(stats[8:9] + stats[9:10])[: ROWS - 128]], axis=0
    ) * (1.0 / D)
    f_third(0)
    normed_grad = s_own[0]
    for k in (1, 2):
        links.wait(y_recv.at[k], f_ss.at[2], f_rs.at[23 + k], p.tid(p.ysrc(k), p.x, c))
        normed_grad = normed_grad + y_recv[k].astype(F32)
    own_gain = jnp.concatenate([gain[pl.ds(2 * t, 1), :], gain[pl.ds(2 * t + 1, 1), :]], axis=1)
    grad[...] = (
        inverse * (own_gain * normed_grad)
        - jnp.concatenate([full_low[t], full_high[t]], axis=1).astype(F32) * (inverse * inverse * inverse * row_stat)
    ).astype(BF16)
    grad_copy = pltpu.make_async_copy(grad, grad_out, local_sem.at[14])
    grad_copy.start()
    most = a_send.at[:, pl.ds(0, N_DP - 1)]
    rollout(most, most, 0, lax.rem(dp + 1, N_DP)).wait_send()
    for tree in trees:
        tree.sent()
    links.sent(w_far, d_ss.at[0], d_rs.at[0], p.partner)
    links.sent(d2_send, d_ss.at[1], d_rs.at[1], p.mate)
    links.sent(kvraw.at[c], d_ss.at[2], d_rs.at[3], p.partner)
    links.sent(e1_send, e_ss.at[0], e_rs.at[0], p.partner)
    links.sent(ebuf.at[pl.ds(0, 3)], e_ss.at[1], e_rs.at[2], p.partner)
    links.sent(rs_all.at[pl.ds(0, 7)], e_ss.at[2], e_rs.at[3], p.partner)
    links.sent(f0_send, f_ss.at[0], f_rs.at[0], p.partner)
    links.sent(f0_send.at[pl.ds(0, 3)], f_ss.at[1], f_rs.at[0], p.partner)
    links.sent(y_send.at[pl.ds(0, 3)], f_ss.at[2], f_rs.at[0], p.partner)
    att_copy.wait()
    grad_copy.wait()


def hand_over(att_in, grad_in, att_out, grad_out, att, grad, sems):
    pairs = ((att_in, att, att_out), (grad_in, grad, grad_out))
    inward = [pltpu.make_async_copy(a, b, sems.at[i]) for i, (a, b, _) in enumerate(pairs)]
    outward = [pltpu.make_async_copy(b, o, sems.at[2 + i]) for i, (_, b, o) in enumerate(pairs)]
    for one in inward:
        one.start()
    for one, two in zip(inward, outward):
        one.wait()
        two.start()
    for two in outward:
        two.wait()


def on_device(
    hidden_slots, lengths, owners, norm_gain, w_query, query_bias, w_keyvalue, keyvalue_bias, grad_attention
):
    frequency = ROPE_BASE ** (-2.0 * np.arange(HALF_DIM, dtype=np.float32) / HEAD_DIM)
    angles = np.arange(WINDOW, dtype=np.float32)[:, None] * frequency[None, :].astype(np.float32)
    angles = np.concatenate([angles, angles], axis=1)
    cosine = jnp.asarray(np.cos(angles), F32)
    sine = jnp.asarray(np.sin(angles), F32)
    operands = (
        hidden_slots, lengths, owners, norm_gain.reshape(64, 128), w_query, query_bias.reshape(2, 128),
        w_keyvalue, keyvalue_bias.reshape(16, 128), grad_attention, cosine, sine,
    )

    def v(*shape, dtype=BF16):
        return pltpu.VMEM(shape, dtype)

    def dma(n):
        return pltpu.SemaphoreType.DMA((n,))

    scratch = [pltpu.VMEM(one.shape, one.dtype) for i, one in enumerate(operands) if i != 6]
    scratch += [v(ROWS, PART), v(ROWS, PART)]
    scratch += [
        pltpu.SMEM((N_DP, N_DP), jnp.int32), v(2, N_DP, WINDOW, 128), v(2, N_DP, WINDOW, 128), v(LANES, ROWS, 128),
        v(LANES, ROWS, 128), v(ROWS, PART, dtype=F32),
        v(ROWS, 128, dtype=F32),
    ]
    scratch += [
        v(2, 2, PART, 512), v(3, PART, 512), v(4, ROWS, 128, dtype=F32),
        v(4, ROWS, 128), v(4, ROWS, 128), v(ROWS, 128), v(ROWS, 128), v(2, ROWS, 128, dtype=F32),
    ]
    scratch += [
        v(ROWS, 128, dtype=F32), v(ROWS, 128, dtype=F32), v(ROWS, PART), v(2, ROWS, 128, dtype=F32),
        v(2, ROWS, 128), v(ROWS, 128), v(ROWS, 128), v(ROWS, 128),
        v(4, GRAD_ROWS, 128), v(256, 128, dtype=F32), v(8, 16, 128, dtype=F32),
        v(4, ROWS, 8 * PART, dtype=F32),
    ]
    scratch += [
        v(4, 4, ROWS, PART), v(4, 4, ROWS, PART), v(4, ROWS, PART), v(4, HALF, PART), v(4, HALF, PART),
        v(4, ROWS, PART), v(4, ROWS, PART), v(4, 2, ROWS, PART), v(4, ROWS, PART, dtype=F32),
        v(4, ROWS, PART, dtype=F32), v(4, ROWS, PART, dtype=F32), v(4, ROWS, PART), v(4, ROWS, PART),
    ]
    scratch += [
        dma(15), dma(1), dma(2), dma(2), dma(2 * TREE_SLOTS), dma(3), dma(4), dma(3), dma(4), dma(3), dma(27),
    ]
    shape = jax.ShapeDtypeStruct((ROWS, PART), BF16)
    outs = pl.pallas_call(
        kernel,
        out_shape=(shape, shape),
        in_specs=[pl.BlockSpec(memory_space=pltpu.HBM)] * len(operands),
        out_specs=[pl.BlockSpec(memory_space=pl.ANY)] * 2,
        scratch_shapes=scratch,
        compiler_params=pltpu.CompilerParams(
            collective_id=0, has_side_effects=True, vmem_limit_bytes=60 * 1024 * 1024
        ),
        name="step",
    )(*operands)
    anywhere = [pl.BlockSpec(memory_space=pltpu.HBM)] * 2
    return pl.pallas_call(
        hand_over,
        out_shape=(shape, shape),
        in_specs=anywhere,
        out_specs=anywhere,
        scratch_shapes=[v(ROWS, PART), v(ROWS, PART), dma(4)],
        compiler_params=pltpu.CompilerParams(vmem_limit_bytes=60 * 1024 * 1024),
        name="hand_over",
    )(*outs)


def solution(mesh):
    in_specs = (
        P("dp", None, "tensor"),
        P(),
        P(),
        P(),
        P(None, "tensor"),
        P("tensor"),
        P("tensor", None),
        P(),
        P("dp", "tensor"),
    )
    out_specs = (P("dp", "tensor"), P("dp", "tensor"))
    return jax.shard_map(on_device, mesh=mesh, in_specs=in_specs, out_specs=out_specs, check_vma=False)
```

```python
import jax
import jax.numpy as jnp
import numpy as np
from jax import lax
from jax.experimental import pallas as pl
from jax.experimental.pallas import tpu as pltpu
from jax.sharding import PartitionSpec as P

D = 8192
HEADS = 64
KV_HEADS = 8
HEAD_DIM = 128
EPSILON = 1e-06
ROPE_BASE = 1000000.0
N_DP = 24
WINDOW = 16
ROWS = 192
HALF = 96
PART = 256
LANES = 32
HALF_DIM = HEAD_DIM // 2
SCALE = HEAD_DIM ** (-0.5)
MESH = pl.DeviceIdType.MESH
F32 = jnp.float32
BF16 = jnp.bfloat16
TREE_SLOTS = 23
GRAD_ROWS = ROWS + 16
ORDER = (1, 2, 3, 0)


def mm(a, b):
    return jnp.dot(a, b, preferred_element_type=F32)


def mm_nt(a, b):
    return lax.dot_general(a, b, (((1,), (1,)), ((), ())), preferred_element_type=F32)


def mm_tn(a, b):
    return lax.dot_general(a, b, (((0,), (0,)), ((), ())), preferred_element_type=F32)


def exact_nt(a, b):
    return lax.dot_general(
        a, b, (((1,), (1,)), ((), ())), preferred_element_type=F32, precision=lax.Precision.HIGHEST
    )


def exact_mm(a, b):
    return lax.dot_general(
        a, b, (((1,), (0,)), ((), ())), preferred_element_type=F32, precision=lax.Precision.HIGHEST
    )


def iota(shape, dim):
    return lax.broadcasted_iota(jnp.int32, shape, dim)


class Links:
    def __init__(self, dp):
        self.dp = dp

    def copy(self, src, dst, send_sem, recv_sem, peer):
        return pltpu.make_async_remote_copy(
            src_ref=src,
            dst_ref=dst,
            send_sem=send_sem,
            recv_sem=recv_sem,
            device_id=(self.dp, peer),
            device_id_type=MESH,
        )

    def send(self, src, dst, send_sem, recv_sem, peer):
        self.copy(src, dst, send_sem, recv_sem, peer).start()

    def wait(self, dst, send_sem, recv_sem, peer):
        self.copy(dst, dst, send_sem, recv_sem, peer).wait_recv()

    def sent(self, bytes_of, send_sem, recv_sem, peer):
        self.copy(bytes_of, bytes_of, send_sem, recv_sem, peer).wait_send()


class Tree:
    def __init__(self, links, place, buffer, cuts, send_sem, recv_sems, base):
        self.links = links
        self.place = place
        self.buffer = buffer
        self.small, self.large = cuts
        self.ss = send_sem
        self.rs = recv_sems
        self.base = base

    def block(self, tid):
        return self.buffer.at[tid]

    def send(self, slot, ref, peer):
        self.links.send(ref, ref, self.ss, self.rs.at[self.base + slot], peer)

    def wait(self, slot, ref, peer):
        self.links.wait(ref, self.ss, self.rs.at[self.base + slot], peer)

    def spread(self, k):
        p = self.place
        ref = self.block(p.tid(p.ysrc(k), p.x, p.c))
        self.send(3 + k, ref, p.mate)
        self.send(7 + k, ref, p.mirror)
        self.send(15 + k, ref, p.partner)

    def start(self):
        p = self.place
        ref = self.block(p.t)
        for k in (1, 2):
            self.send(k - 1, ref, p.tid(p.ydst(k), p.x, p.c))
        self.spread(0)

    def step_y(self, k):
        p = self.place
        ref = self.block(p.tid(p.ysrc(k), p.x, p.c))
        self.wait(k - 1, ref, p.tid(p.ysrc(k), p.x, p.c))
        if k == 2:
            self.send(2, ref, p.tid(p.ydst(1), p.x, p.c))
        self.spread(k)

    def step_mate(self, k):
        p = self.place
        tid = p.tid(p.ysrc(k), p.x + 1 - 2 * p.kind, p.c)
        self.wait(3 + k, self.block(tid), p.mate)
        rows = pl.ds(pl.multiple_of((1 - p.kind) * self.large, 16), self.small)
        self.send(11 + k, self.buffer.at[tid, rows], p.mirror)
        self.send(15 + k, self.block(tid), p.partner)

    def step_mirror(self, k):
        p = self.place
        tid = p.tid(p.ysrc(k), 3 - p.x, p.c)
        self.wait(7 + k, self.block(tid), p.mirror)
        rows = pl.ds(pl.multiple_of(p.kind * self.small, 16), self.large)
        self.send(11 + k, self.buffer.at[tid, rows], p.mate)
        self.send(15 + k, self.block(tid), p.partner)

    def step_far(self, k):
        p = self.place
        tid = p.tid(p.ysrc(k), p.xat(2), p.c)
        self.wait(11 + k, self.block(tid), p.left)
        self.send(19 + k, self.block(tid), p.partner)

    def partner_near(self, k):
        self.wait(15 + k, self.buffer.at[pl.ds(0, 3)], self.place.partner)

    def partner_far(self, k):
        p = self.place
        self.wait(19 + k, self.block(p.tid(p.ysrc(k), p.xat(2), 1 - p.c)), p.partner)

    def sent(self):
        self.links.sent(self.buffer.at[pl.ds(0, 31)], self.ss, self.rs.at[self.base], self.place.partner)


class Place:
    def __init__(self):
        self.dp = lax.axis_index("dp")
        self.t = lax.axis_index("tensor")
        self.c = lax.rem(self.t, 2)
        self.x = lax.rem(lax.div(self.t, 2), 4)
        self.y = lax.div(self.t, 8)
        self.left = self.tid(self.y, self.xat(3), self.c)
        self.right = self.tid(self.y, self.xat(1), self.c)
        self.partner = self.tid(self.y, self.x, 1 - self.c)
        self.pair = lax.div(self.x, 2)
        self.kind = lax.rem(self.x, 2)
        self.mirror = self.tid(self.y, 3 - self.x, self.c)
        self.mirror_other = self.tid(self.y, 3 - self.x, 1 - self.c)
        self.row_index = self.x * 2 + self.c
        self.mate = self.tid(self.y, self.x + 1 - 2 * self.kind, self.c)

    def in_row(self, j):
        return self.y * 8 + lax.rem(self.row_index + j, 8)

    def tid(self, y, x, c):
        return (y * 4 + x) * 2 + c

    def xat(self, shift):
        return lax.rem(self.x + shift, 4)

    def ydst(self, k):
        if k == 3:
            return 3 - self.y
        if k == 2:
            return self.y + 2 - 4 * lax.div(self.y, 2)
        if k == 1:
            return self.y + 1 - 2 * lax.rem(self.y, 2)
        return self.y

    def ysrc(self, k):
        return self.ydst(k)


def kernel(
    slots_in, lengths_in, owners_in, gain_in, wq_in, qbias_in, wkv_in, kvbias_in, up_in, cos_in, sin_in,
    att_out, grad_out,
    slots, lengths, owners, gain, wq, qbias, kvbias, up, cos16, sin16, att, grad,
    owner_table, a_send, a_recv, full_low, full_high, acc, ssq,
    w_own, w_far, d_own, d2_send, d2_recv, d3_send, d3_recv, kvraw,
    cos_s, sin_s, q_grad, kv_f32, e1_send, e1_recv, e2_send, e2_recv, ebuf, rs_rows, rs_all, products_s,
    f0_send, f0_recv, far_send, from_mate, from_mirror, mate_send, mirror_send, column_in, s_own, s_mate, s_mirror, y_send, y_recv,
    local_sem, a_ss, a_rs, b_ss, b_rs, d_ss, d_rs, e_ss, e_rs, f_ss, f_rs,
):
    p = Place()
    dp, t, c = p.dp, p.t, p.c

    pairs = (
        (owners_in, owner_table), (slots_in, slots), (owners_in, owners), (lengths_in, lengths), (gain_in, gain),
        (kvbias_in, kvbias), (qbias_in, qbias), (cos_in, cos16), (sin_in, sin16), (up_in, up), (wq_in, wq),
    )
    loads = [pltpu.make_async_copy(a, b, local_sem.at[i]) for i, (a, b) in enumerate(pairs)]
    weight_loads = []
    for kind in (0, 1):
        for pair in (0, 1):
            for i in range(4):
                weight_loads.append(
                    pltpu.make_async_copy(
                        wkv_in.at[:, pl.ds(kind * 1024 + (2 * i + pair) * 128, 128)],
                        w_own.at[kind, pair, :, pl.ds(i * 128, 128)],
                        local_sem.at[12],
                    )
                )
    for one in loads[:2]:
        one.start()

    barrier = pltpu.get_barrier_semaphore()

    half_index, depth = lax.div(dp, 12), lax.rem(dp, 12)
    offsets = [(dh, dz) for dh in (0, 1) for dz in range(12) if dh or dz]
    offsets.sort(key=lambda o: -(4 * o[0] + min(o[1], 12 - o[1])))
    batch_peers = [lax.rem(half_index + dh, 2) * 12 + lax.rem(depth + dz, 12) for dh, dz in offsets]
    for peer in batch_peers:
        pl.semaphore_signal(barrier, inc=1, device_id=(peer, t), device_id_type=MESH)
    for peer in tuple(p.in_row(j) for j in range(1, 8)) + tuple(p.tid(p.ydst(k), p.x, c) for k in (1, 2, 3)):
        pl.semaphore_signal(barrier, inc=1, device_id=(dp, peer), device_id_type=MESH)

    for one in loads[2:] + weight_loads:
        one.start()

    total = N_DP * WINDOW
    loads[0].wait()
    slot_of = []
    for b in range(N_DP):
        found = jnp.int32(0)
        for j in range(1, N_DP):
            found = jnp.where(owner_table[b, j] == dp, j, found)
        slot_of.append(found)
    loads[1].wait()
    for b in range(N_DP):
        block = slots[slot_of[b]]
        for h in (0, 1):
            a_send[h, b] = block[:, h * 128 : h * 128 + 128]
    for h in (0, 1):
        a_recv[h, dp] = a_send[h, dp]
    pl.semaphore_wait(barrier, N_DP - 1 + 10)

    def rollout(src, dst, k, peer):
        return pltpu.make_async_remote_copy(
            src_ref=src, dst_ref=dst, send_sem=a_ss.at[0], recv_sem=a_rs.at[k], device_id=(peer, t), device_id_type=MESH
        )

    def wait_rollout(h):
        most = a_recv.at[h, pl.ds(0, N_DP - 1)]
        rollout(most, most, h, lax.rem(dp + 1, N_DP)).wait_recv()

    for h in (0, 1):
        for peer in batch_peers:
            rollout(a_send.at[h, peer], a_recv.at[h, dp], h, peer).start()

    pltpu.make_async_copy(w_own, w_own, local_sem.at[12]).wait()
    for one in loads[2:]:
        one.wait()
    links = Links(dp)
    links.send(w_own.at[1 - c, p.pair], w_far.at[0], d_ss.at[0], d_rs.at[0], p.partner)
    links.send(w_own.at[c, 1 - p.pair], w_far.at[1], d_ss.at[0], d_rs.at[0], p.mirror)
    links.send(w_own.at[1 - c, 1 - p.pair], w_far.at[2], d_ss.at[0], d_rs.at[0], p.mirror_other)

    length_row = jnp.broadcast_to(lengths[pl.ds(dp, 1), :].astype(F32), (ROWS, N_DP))
    owner_row = jnp.broadcast_to(owners[pl.ds(dp, 1), :].astype(F32), (ROWS, N_DP))
    before = (iota((N_DP, N_DP), 0) < iota((N_DP, N_DP), 1)).astype(F32).astype(BF16)
    starts = mm(length_row.astype(BF16), before)
    place = iota((ROWS, N_DP), 0).astype(F32)
    inside = (place >= starts) & (place < starts + length_row)
    start = jnp.sum(jnp.where(inside, starts, 0.0), axis=1, keepdims=True)
    source = jnp.sum(jnp.where(inside, owner_row, 0.0), axis=1, keepdims=True)
    offset = iota((ROWS, 1), 0).astype(F32) - start
    wanted = (source * WINDOW + offset).astype(jnp.int32)
    select = (iota((ROWS, total), 1) == wanted).astype(F32).astype(BF16)
    turn = (iota((ROWS, WINDOW), 1) == offset.astype(jnp.int32)).astype(F32)
    sign = jnp.where(iota((ROWS, HEAD_DIM), 1) < HALF_DIM, -1.0, 1.0)
    cos_s[...] = exact_mm(turn, cos16[...])
    sin_s[...] = exact_mm(turn, sin16[...])
    key_place = iota((ROWS, ROWS), 1)
    allowed = (key_place >= start.astype(jnp.int32)) & (key_place <= iota((ROWS, ROWS), 0))
    acc[...] = jnp.zeros_like(acc)
    ssq[...] = jnp.zeros_like(ssq)
    trees = [
        Tree(links, p, ref, (96, 96), b_ss.at[h], b_rs, h * TREE_SLOTS) for h, ref in enumerate((full_low, full_high))
    ]
    for h, ref in enumerate((full_low, full_high)):
        wait_rollout(h)
        ref[t] = mm(select, a_recv[h].reshape(total, 128)).astype(BF16)
        trees[h].start()

    def steps(name, k):
        for tree in trees:
            getattr(tree, name)(k)

    def scaled(tid):
        low, high = full_low[tid].astype(F32), full_high[tid].astype(F32)
        value = jnp.concatenate([low * gain[pl.ds(2 * tid, 1), :], high * gain[pl.ds(2 * tid + 1, 1), :]], axis=1)
        return value.astype(BF16), low * low + high * high

    def consume(*items):
        total, squares = None, None
        for core, k, shifts in items:
            for shift in shifts:
                tid = p.tid(p.ysrc(k), p.xat(shift), core)
                value, square = scaled(tid)
                part = mm(value, wq[pl.ds(pl.multiple_of(tid * PART, PART), PART), :])
                total = part if total is None else total + part
                squares = square if squares is None else squares + square
        ssq[...] += squares
        acc[...] += total

    near, far = (0, 1, 3), (2,)
    first, second = trees
    first.step_mate(0)
    first.step_y(1)
    first.step_mirror(0)
    first.step_y(2)
    second.step_mate(0)
    second.step_y(1)
    second.step_mirror(0)
    second.step_y(2)
    first.step_mate(1)
    first.step_y(3)
    steps("partner_near", 0)
    links.wait(w_far, d_ss.at[0], d_rs.at[0], p.partner)
    weights_of = ((t, w_own.at[c, p.pair]), (p.partner, w_far.at[0]), (p.mirror, w_far.at[1]), (p.mirror_other, w_far.at[2]))
    low_sum, high_sum = jnp.zeros((ROWS, 256), F32), jnp.zeros((ROWS, 256), F32)
    for tid, ref in weights_of:
        value = scaled(tid)[0]
        low_sum = low_sum + mm(value, ref[:, :256])
        high_sum = high_sum + mm(value, ref[:, 256:])
    for i, value in enumerate((low_sum, high_sum)):
        d_own[2 * i] = value[:, :128]
        d_own[2 * i + 1] = value[:, 128:]
    for k in (1, 2, 3):
        d2_send[k] = d_own[p.ydst(k)].astype(BF16)
        links.send(d2_send.at[k], d2_recv.at[k], d_ss.at[1], d_rs.at[1], p.tid(p.ydst(k), p.x, c))
    first.step_mirror(1)
    second.step_mate(1)
    second.step_y(3)
    second.step_mirror(1)
    steps("step_far", 0)
    consume((c, 0, near), (1 - c, 0, near))
    first.step_mate(2)
    first.step_mirror(2)
    second.step_mate(2)
    second.step_mirror(2)
    steps("step_far", 1)
    consume((c, 1, near))
    column = d_own[p.y]
    links.wait(d2_recv.at[pl.ds(1, 3)], d_ss.at[1], d_rs.at[1], p.mate)
    for k in (1, 2, 3):
        column = column + d2_recv[k].astype(F32)
    d3_send[...] = column.astype(BF16)
    links.send(d3_send, d3_recv, d_ss.at[1], d_rs.at[2], p.mate)
    steps("partner_near", 1)
    consume((1 - c, 1, near))
    steps("step_mate", 3)
    steps("step_mirror", 3)
    steps("step_far", 2)
    consume((c, 2, near), (c, 0, far))
    steps("partner_near", 2)
    steps("partner_far", 0)
    consume((1 - c, 2, near), (1 - c, 0, far))
    consume((c, 3, near))
    steps("step_far", 3)
    links.wait(d3_recv, d_ss.at[1], d_rs.at[2], p.mate)
    kvraw[c] = column + d3_recv[...].astype(F32)
    links.send(kvraw.at[c], kvraw.at[c], d_ss.at[2], d_rs.at[3], p.partner)
    consume((c, 1, far), (c, 2, far), (c, 3, far))
    steps("partner_near", 3)
    steps("partner_far", 1)
    steps("partner_far", 2)
    consume((1 - c, 3, near), (1 - c, 1, far), (1 - c, 2, far))
    steps("partner_far", 3)
    consume((1 - c, 3, far))
    links.wait(kvraw.at[1 - c], d_ss.at[2], d_rs.at[3], p.partner)

    cosine, sine = cos_s[...], sin_s[...]
    inverse = lax.rsqrt(jnp.sum(ssq[...], axis=1, keepdims=True) * (1.0 / D) + EPSILON)

    def rotate(u):
        return u * cosine + pltpu.roll(u, HALF_DIM, 1) * (sign * sine)

    def unrotate(z, cosine, sine, sign):
        return z * cosine - pltpu.roll(z * sine, HALF_DIM, 1) * sign

    group = p.y * 2 + p.pair
    key_raw, value_raw = kvraw[0], kvraw[1]
    key = rotate(inverse * key_raw + kvbias[pl.ds(group, 1), :]).astype(BF16)
    value = (inverse * value_raw + kvbias[pl.ds(KV_HEADS + group, 1), :]).astype(BF16)
    query = jnp.concatenate(
        [rotate(inverse * acc[:, h * 128 : h * 128 + 128] + qbias[h : h + 1, :]).astype(BF16) for h in (0, 1)], axis=0
    )
    upstream = jnp.concatenate([up[:, :128], up[:, 128:]], axis=0)
    both = jnp.concatenate([allowed.astype(F32), allowed.astype(F32)], axis=0) > 0.5
    scores = jnp.where(both, mm_nt(query, key) * SCALE, -1e30)
    highest = jnp.max(scores, axis=1, keepdims=True)
    exponent = jnp.where(both, jnp.exp(scores - highest), 0.0)
    weights = exponent * (1.0 / jnp.sum(exponent, axis=1, keepdims=True))
    low = weights.astype(BF16)
    weight_grad = mm_nt(upstream, value)
    inner = jnp.sum(weights * weight_grad, axis=1, keepdims=True)
    score_grad = (weights * (weight_grad - inner) * SCALE).astype(BF16)
    query_grad = mm(score_grad, key)
    for h in (0, 1):
        piece = unrotate(query_grad[h * ROWS : h * ROWS + ROWS], cosine, sine, sign).astype(BF16)
        q_grad[:, h * 128 : h * 128 + 128] = piece

    def products(k):
        rows = pl.ds(pl.multiple_of(p.ydst(k) * (8 * PART), 8 * PART), 8 * PART)
        products_s[k] = mm_nt(q_grad[...], wq[rows, :])

    def partial(k, shift, core):
        col = (lax.rem(p.x + shift, 4) * 2 + core) * PART
        return products_s[k, :, pl.ds(pl.multiple_of(col, PART), PART)]

    kind = p.kind
    far_shift, mate_shift, mirror_shift = 2, 1 + 2 * kind, 3 - 2 * kind

    def rows_of(index):
        return pl.ds(pl.multiple_of(index * HALF, HALF), HALF)

    def f_core(k, shift, sem, more=None):
        value = partial(k, shift, 1 - c)
        if more is not None:
            value = value + more
        f0_send[k, shift] = value.astype(BF16)
        links.send(f0_send.at[k, shift], f0_recv.at[k, shift], f_ss.at[0], f_rs.at[sem], p.partner)

    def f_cores_far(k):
        f_core(k, far_shift, k)

    def f_cores_mate(k):
        f_core(k, mate_shift, 4 + k)

    def f_cores_rest(k):
        f_core(k, mirror_shift, 8 + k)
        f_core(k, 0, 8 + k)

    def chip_sum(k, shift):
        return partial(k, shift, c) + f0_recv[k, shift].astype(F32)

    def f_far(k):
        links.wait(f0_recv.at[k, 2], f_ss.at[0], f_rs.at[k], p.partner)
        far_send[k] = chip_sum(k, far_shift).astype(BF16)
        links.send(far_send.at[k, rows_of(kind)], from_mate.at[k], f_ss.at[1], f_rs.at[12 + k], p.mate)
        links.send(far_send.at[k, rows_of(1 - kind)], from_mirror.at[k], f_ss.at[1], f_rs.at[16 + k], p.mirror)

    def f_mate(k):
        links.wait(f0_recv.at[k, 1], f_ss.at[0], f_rs.at[4 + k], p.partner)
        s_mate[k] = chip_sum(k, mate_shift)
        mate_send[k, rows_of(1 - kind)] = s_mate[k, rows_of(1 - kind)].astype(BF16)
        one = mate_send.at[k, rows_of(1 - kind)]
        links.send(one, column_in.at[k, 0, rows_of(1 - kind)], f_ss.at[1], f_rs.at[20 + k], p.mate)

    def f_rest(k, mirror_more=None, own_more=None):
        links.wait(f0_recv.at[k, pl.ds(0, 2)], f_ss.at[0], f_rs.at[8 + k], p.partner)
        value = chip_sum(k, mirror_shift)
        s_mirror[k] = value if mirror_more is None else value + mirror_more
        mirror_send[k, rows_of(kind)] = s_mirror[k, rows_of(kind)].astype(BF16)
        one = mirror_send.at[k, rows_of(kind)]
        links.send(one, column_in.at[k, 1, rows_of(kind)], f_ss.at[1], f_rs.at[20 + k], p.mirror)
        value = chip_sum(k, 0)
        s_own[k] = value if own_more is None else value + own_more

    def f_relay_mate(k):
        links.wait(from_mirror.at[k], f_ss.at[1], f_rs.at[16 + k], p.mirror)
        mate_send[k, rows_of(kind)] = (s_mate[k, rows_of(kind)] + from_mirror[k].astype(F32)).astype(BF16)
        one = mate_send.at[k, rows_of(kind)]
        links.send(one, column_in.at[k, 0, rows_of(kind)], f_ss.at[1], f_rs.at[20 + k], p.mate)

    def f_relay_mirror(k):
        links.wait(from_mate.at[k], f_ss.at[1], f_rs.at[12 + k], p.mate)
        mirror_send[k, rows_of(1 - kind)] = (s_mirror[k, rows_of(1 - kind)] + from_mate[k].astype(F32)).astype(BF16)
        one = mirror_send.at[k, rows_of(1 - kind)]
        links.send(one, column_in.at[k, 1, rows_of(1 - kind)], f_ss.at[1], f_rs.at[20 + k], p.mirror)

    def f_third(k):
        links.wait(column_in.at[k], f_ss.at[1], f_rs.at[20 + k], p.mate)
        value = s_own[k] + column_in[k, 0].astype(F32) + column_in[k, 1].astype(F32)
        if k == 0:
            s_own[k] = value
        else:
            if k == 2:
                links.wait(y_recv.at[3], f_ss.at[2], f_rs.at[26], p.tid(p.ydst(1), p.x, c))
                value = value + y_recv[3].astype(F32)
            y_send[k] = value.astype(BF16)
            peer = p.tid(p.ydst(2 if k == 2 else 1), p.x, c)
            links.send(y_send.at[k], y_recv.at[k], f_ss.at[2], f_rs.at[23 + k], peer)

    far_tid = p.tid(p.ydst(3), p.xat(2), 1 - c)
    far_rows = pl.ds(pl.multiple_of(far_tid * PART, PART), PART)
    f0_send[3, 2] = mm_nt(q_grad[...], wq[far_rows, :]).astype(BF16)
    links.send(f0_send.at[3, 2], f0_recv.at[3, 2], f_ss.at[0], f_rs.at[3], p.partner)
    products(3)
    kv_f32[0] = mm_tn(score_grad, query)
    kv_f32[1] = mm_tn(low, upstream)
    e1_send[...] = kv_f32[...].astype(BF16)
    links.send(e1_send.at[1 - c], e1_recv, e_ss.at[0], e_rs.at[0], p.partner)
    f_cores_mate(3)
    f_cores_rest(3)
    attended = mm(low, value).astype(BF16)
    att[:, :128] = attended[:ROWS]
    att[:, 128:] = attended[ROWS:]
    att_copy = pltpu.make_async_copy(att, att_out, local_sem.at[13])
    att_copy.start()
    for h in (0, 1):
        inner_part = q_grad[:, h * 128 : h * 128 + 128].astype(F32) * acc[:, h * 128 : h * 128 + 128]
        if h == 0:
            rs_rows[pl.ds(0, ROWS), :] = inner_part
        else:
            rs_rows[pl.ds(0, ROWS), :] += inner_part
    rs_rows[pl.ds(ROWS, 64), :] = jnp.zeros((64, 128), F32)
    f_far(3)
    links.wait(e1_recv, e_ss.at[0], e_rs.at[0], p.partner)
    chip_grad = kv_f32[c] + e1_recv[...].astype(F32)
    e2_send[...] = chip_grad.astype(BF16)
    links.send(e2_send, e2_recv, e_ss.at[0], e_rs.at[1], p.mate)
    f_mate(3)
    products(2)
    f_cores_far(2)
    f_cores_mate(2)
    f_cores_rest(2)
    f_rest(3)
    f_far(2)
    f_mate(2)
    f_rest(2)
    f_relay_mate(3)
    f_relay_mirror(3)
    links.wait(e2_recv, e_ss.at[0], e_rs.at[1], p.mate)
    value_side = c.astype(F32)
    finished = unrotate(
        kv_f32[c] + e1_recv[...].astype(F32) + e2_recv[...].astype(F32),
        cosine * (1.0 - value_side) + value_side,
        sine * (1.0 - value_side),
        sign,
    ).astype(BF16)
    rs_rows[pl.ds(0, ROWS), :] += 0.5 * finished.astype(F32) * kvraw[c]
    ones = jnp.ones((8, 128), F32)
    stat = jnp.concatenate([exact_nt(ones, rs_rows[0:128, :]), exact_nt(ones, rs_rows[128:256, :])], axis=0)
    coarse = stat.astype(BF16).astype(F32)
    ebuf[p.y, pl.ds(0, ROWS)] = finished
    ebuf[p.y, pl.ds(ROWS, 16)] = jnp.where(lax.rem(iota((16, 128), 0), 2) == 0, coarse, stat - coarse).astype(BF16)
    for k in (1, 2, 3):
        links.send(ebuf.at[p.y], ebuf.at[p.y], e_ss.at[1], e_rs.at[2], p.tid(p.ydst(k), p.x, c))
    products(1)
    f_cores_far(1)
    f_cores_mate(1)
    f_cores_rest(1)
    f_far(1)
    f_relay_mate(2)
    f_relay_mirror(2)
    products(0)
    f_cores_far(0)
    f_cores_mate(0)
    f_mate(1)
    f_rest(1)
    f_third(3)
    f_relay_mate(1)
    f_relay_mirror(1)
    f_far(0)
    f_mate(0)
    links.wait(ebuf.at[pl.ds(0, 3)], e_ss.at[1], e_rs.at[2], p.partner)
    pair_grads = jnp.concatenate([ebuf[i, pl.ds(0, ROWS)] for i in range(4)], axis=1)
    (_, w_me), (_, w_partner), (_, w_mirror), (_, w_mirror_other) = weights_of
    f_core(0, mirror_shift, 8, mm_nt(pair_grads, w_mirror_other[...]))
    f_core(0, 0, 8, mm_nt(pair_grads, w_partner[...]))
    row_sum = jnp.zeros((16, 128), F32)
    for i in range(4):
        row_sum = row_sum + ebuf[i, pl.ds(ROWS, 16)].astype(F32)
    rs_all[p.row_index] = row_sum
    for j in range(1, 8):
        own_row = rs_all.at[p.row_index]
        links.send(own_row, own_row, e_ss.at[2], e_rs.at[3], p.in_row(j))
    mirror_part = mm_nt(pair_grads, w_mirror[...])
    own_part = mm_nt(pair_grads, w_me[...])
    f_rest(0, mirror_part, own_part)
    f_third(2)
    f_third(1)
    f_relay_mate(0)
    f_relay_mirror(0)
    f_third(0)
    links.wait(rs_all.at[pl.ds(0, 7)], e_ss.at[2], e_rs.at[3], p.partner)
    stats = rs_all[0]
    for j in range(1, 8):
        stats = stats + rs_all[j]
    eye = iota((128, 128), 0) == iota((128, 128), 1)

    def upright(row):
        return jnp.sum(jnp.where(eye, jnp.broadcast_to(row, (128, 128)), 0.0), axis=1, keepdims=True)

    row_stat = jnp.concatenate(
        [upright(stats[0:1] + stats[1:2]), upright(stats[8:9] + stats[9:10])[: ROWS - 128]], axis=0
    ) * (1.0 / D)
    normed_grad = s_own[0]
    for k in (1, 2):
        links.wait(y_recv.at[k], f_ss.at[2], f_rs.at[23 + k], p.tid(p.ysrc(k), p.x, c))
        normed_grad = normed_grad + y_recv[k].astype(F32)
    own_gain = jnp.concatenate([gain[pl.ds(2 * t, 1), :], gain[pl.ds(2 * t + 1, 1), :]], axis=1)
    grad[...] = (
        inverse * (own_gain * normed_grad)
        - jnp.concatenate([full_low[t], full_high[t]], axis=1).astype(F32) * (inverse * inverse * inverse * row_stat)
    ).astype(BF16)
    grad_copy = pltpu.make_async_copy(grad, grad_out, local_sem.at[14])
    grad_copy.start()
    most = a_send.at[:, pl.ds(0, N_DP - 1)]
    rollout(most, most, 0, lax.rem(dp + 1, N_DP)).wait_send()
    for tree in trees:
        tree.sent()
    links.sent(w_far, d_ss.at[0], d_rs.at[0], p.partner)
    links.sent(d2_send, d_ss.at[1], d_rs.at[1], p.mate)
    links.sent(kvraw.at[c], d_ss.at[2], d_rs.at[3], p.partner)
    links.sent(e1_send, e_ss.at[0], e_rs.at[0], p.partner)
    links.sent(ebuf.at[pl.ds(0, 3)], e_ss.at[1], e_rs.at[2], p.partner)
    links.sent(rs_all.at[pl.ds(0, 7)], e_ss.at[2], e_rs.at[3], p.partner)
    links.sent(f0_send, f_ss.at[0], f_rs.at[0], p.partner)
    links.sent(f0_send.at[pl.ds(0, 3)], f_ss.at[1], f_rs.at[0], p.partner)
    links.sent(y_send.at[pl.ds(0, 3)], f_ss.at[2], f_rs.at[0], p.partner)
    att_copy.wait()
    grad_copy.wait()


def hand_over(att_in, grad_in, att_out, grad_out, att, grad, sems):
    pairs = ((att_in, att, att_out), (grad_in, grad, grad_out))
    inward = [pltpu.make_async_copy(a, b, sems.at[i]) for i, (a, b, _) in enumerate(pairs)]
    outward = [pltpu.make_async_copy(b, o, sems.at[2 + i]) for i, (_, b, o) in enumerate(pairs)]
    for one in inward:
        one.start()
    for one, two in zip(inward, outward):
        one.wait()
        two.start()
    for two in outward:
        two.wait()


def on_device(
    hidden_slots, lengths, owners, norm_gain, w_query, query_bias, w_keyvalue, keyvalue_bias, grad_attention
):
    frequency = ROPE_BASE ** (-2.0 * np.arange(HALF_DIM, dtype=np.float32) / HEAD_DIM)
    angles = np.arange(WINDOW, dtype=np.float32)[:, None] * frequency[None, :].astype(np.float32)
    angles = np.concatenate([angles, angles], axis=1)
    cosine = jnp.asarray(np.cos(angles), F32)
    sine = jnp.asarray(np.sin(angles), F32)
    operands = (
        hidden_slots, lengths, owners, norm_gain.reshape(64, 128), w_query, query_bias.reshape(2, 128),
        w_keyvalue, keyvalue_bias.reshape(16, 128), grad_attention, cosine, sine,
    )

    def v(*shape, dtype=BF16):
        return pltpu.VMEM(shape, dtype)

    def dma(n):
        return pltpu.SemaphoreType.DMA((n,))

    scratch = [pltpu.VMEM(one.shape, one.dtype) for i, one in enumerate(operands) if i != 6]
    scratch += [v(ROWS, PART), v(ROWS, PART)]
    scratch += [
        pltpu.SMEM((N_DP, N_DP), jnp.int32), v(2, N_DP, WINDOW, 128), v(2, N_DP, WINDOW, 128), v(LANES, ROWS, 128),
        v(LANES, ROWS, 128), v(ROWS, PART, dtype=F32),
        v(ROWS, 128, dtype=F32),
    ]
    scratch += [
        v(2, 2, PART, 512), v(3, PART, 512), v(4, ROWS, 128, dtype=F32),
        v(4, ROWS, 128), v(4, ROWS, 128), v(ROWS, 128), v(ROWS, 128), v(2, ROWS, 128, dtype=F32),
    ]
    scratch += [
        v(ROWS, 128, dtype=F32), v(ROWS, 128, dtype=F32), v(ROWS, PART), v(2, ROWS, 128, dtype=F32),
        v(2, ROWS, 128), v(ROWS, 128), v(ROWS, 128), v(ROWS, 128),
        v(4, GRAD_ROWS, 128), v(256, 128, dtype=F32), v(8, 16, 128, dtype=F32),
        v(4, ROWS, 8 * PART, dtype=F32),
    ]
    scratch += [
        v(4, 4, ROWS, PART), v(4, 4, ROWS, PART), v(4, ROWS, PART), v(4, HALF, PART), v(4, HALF, PART),
        v(4, ROWS, PART), v(4, ROWS, PART), v(4, 2, ROWS, PART), v(4, ROWS, PART, dtype=F32),
        v(4, ROWS, PART, dtype=F32), v(4, ROWS, PART, dtype=F32), v(4, ROWS, PART), v(4, ROWS, PART),
    ]
    scratch += [
        dma(15), dma(1), dma(2), dma(2), dma(2 * TREE_SLOTS), dma(3), dma(4), dma(3), dma(4), dma(3), dma(27),
    ]
    shape = jax.ShapeDtypeStruct((ROWS, PART), BF16)
    outs = pl.pallas_call(
        kernel,
        out_shape=(shape, shape),
        in_specs=[pl.BlockSpec(memory_space=pltpu.HBM)] * len(operands),
        out_specs=[pl.BlockSpec(memory_space=pl.ANY)] * 2,
        scratch_shapes=scratch,
        compiler_params=pltpu.CompilerParams(
            collective_id=0, has_side_effects=True, vmem_limit_bytes=60 * 1024 * 1024
        ),
        name="step",
    )(*operands)
    anywhere = [pl.BlockSpec(memory_space=pltpu.HBM)] * 2
    return pl.pallas_call(
        hand_over,
        out_shape=(shape, shape),
        in_specs=anywhere,
        out_specs=anywhere,
        scratch_shapes=[v(ROWS, PART), v(ROWS, PART), dma(4)],
        compiler_params=pltpu.CompilerParams(vmem_limit_bytes=60 * 1024 * 1024),
        name="hand_over",
    )(*outs)


def solution(mesh):
    in_specs = (
        P("dp", None, "tensor"),
        P(),
        P(),
        P(),
        P(None, "tensor"),
        P("tensor"),
        P("tensor", None),
        P(),
        P("dp", "tensor"),
    )
    out_specs = (P("dp", "tensor"), P("dp", "tensor"))
    return jax.shard_map(on_device, mesh=mesh, in_specs=in_specs, out_specs=out_specs, check_vma=False)
```
